256 devices in a mesh: band: 32 (over z, x_hi, core), lane: 8 (over y, x_lo).
Axes of the slice: x: 4 (x_hi: 2, x_lo: 2; x = x_hi * 2 + x_lo), y: 4, z: 8, core: 2. Of those that a mesh axis runs over, the one named last changes fastest.
Arguments:
- load_terms: float32 [2048, 512, 256], P('band', 'lane'), may hold values from -6 to 6
- start_values: float32 [2048, 512, 256], P('band', 'lane'), may hold values from -6 to 6
- reaction_rate: float32 [2048, 512, 256], P('band', 'lane'), may hold values from 0.1 to 0.9
Outputs:
- solution: float32 [2048, 512, 256], P('band', 'lane')
- remaining: float32 [2048, 512, 256], P('band', 'lane')
The draws below stay inside these ranges and needn't reach their ends.
All inputs are finite; a program needn't handle non-finite values.
Results may differ from the reference program's by a relative error of at most 0.0003.
Values sent between devices are 32-bit elements.
A program may use at most 128 MiB of HBM per device.

```python
import jax
import jax.numpy as jnp
from jax import lax

LAYERS = 256
RATIO = 2
BEFORE = 3
AFTER = 2
INNER = 13
GRID_Y = 2048
GRID_X = 512


def levels(key, dims, shards, smallest, high):
    factor_of, own = 1.0, jax.random.fold_in(key, 6)
    for axis_at, shards_of in shards:
        steps = jnp.exp(jax.random.uniform(jax.random.fold_in(own, axis_at), (shards_of,), jnp.float32, smallest / len(shards), high / len(shards)))
        factor_of = factor_of * jnp.repeat(steps, dims[axis_at] // shards_of).reshape([-1 if axis == axis_at else 1 for axis in range(len(dims))])
    return factor_of


def gaussian(own_key, shape, width, bound, cuts=(), kind=jnp.bfloat16):
    level = levels(own_key, shape, cuts, -0.22, 0.18) if cuts else 1.0
    entries = jax.random.normal(own_key, shape, jnp.float32) * width * level
    return jnp.minimum(jnp.maximum(entries, -bound), bound).astype(kind)


def setup_inputs(seed: int = 0) -> dict:
    seeds = jax.random.split(jax.random.key(seed), 4)
    load_terms = gaussian(seeds[0], (GRID_Y, GRID_X, LAYERS), 1.0, 6.0, ((0, 32), (1, 8)), jnp.float32)
    start_values = gaussian(seeds[1], (GRID_Y, GRID_X, LAYERS), 1.0, 6.0, ((0, 32), (1, 8)), jnp.float32)
    reaction_rate = jnp.clip(0.1 + 0.79999997 * jax.random.uniform(seeds[2], (GRID_Y, GRID_X, LAYERS), jnp.float32) ** levels(seeds[2], (GRID_Y, GRID_X, LAYERS), ((0, 32), (1, 8)), -0.2, 0.2), 0.1, 0.9)
    return dict(load_terms=load_terms, start_values=start_values, reaction_rate=reaction_rate)


def cross_sum(padded):
    inner_y, inner_x = padded.shape[0] - 2, padded.shape[1] - 2
    middle_rows = lax.slice_in_dim(padded, 1, 1 + inner_y, axis=0)
    middle_columns = lax.slice_in_dim(padded, 1, 1 + inner_x, axis=1)
    return (lax.slice_in_dim(middle_columns, 0, inner_y, axis=0) + lax.slice_in_dim(middle_columns, 2, 2 + inner_y, axis=0)
            + lax.slice_in_dim(middle_rows, 0, inner_x, axis=1) + lax.slice_in_dim(middle_rows, 2, 2 + inner_x, axis=1))


def smooth_step(padded, values, load, mass_here):
    return values + 0.8 * (load + cross_sum(padded) - (4.0 + mass_here) * values) / (4.0 + mass_here)


def block_means(values):
    cut = values.reshape(values.shape[0] // RATIO, RATIO, values.shape[1] // RATIO, RATIO, values.shape[2])
    return jnp.mean(cut, axis=(1, 3))


def spread_blocks(values):
    return jnp.repeat(jnp.repeat(values, RATIO, axis=0), RATIO, axis=1)


def reference(load_terms, start_values, reaction_rate):
    values = start_values
    for sweep in range(BEFORE):
        values = smooth_step(jnp.pad(values, ((1, 1), (1, 1), (0, 0)), mode="constant"), values, load_terms, reaction_rate)
    defect = load_terms + cross_sum(jnp.pad(values, ((1, 1), (1, 1), (0, 0)), mode="constant")) - (4.0 + reaction_rate) * values
    coarse_load, coarse_mass = block_means(defect) * RATIO, block_means(reaction_rate) * RATIO
    coarse_values = jnp.zeros_like(coarse_load)
    for sweep in range(INNER):
        coarse_values = smooth_step(jnp.pad(coarse_values, ((1, 1), (1, 1), (0, 0)), mode="constant"), coarse_values, coarse_load, coarse_mass)
    values = values + spread_blocks(coarse_values)
    for sweep in range(AFTER):
        values = smooth_step(jnp.pad(values, ((1, 1), (1, 1), (0, 0)), mode="constant"), values, load_terms, reaction_rate)
    solution = values
    remaining = load_terms + cross_sum(jnp.pad(solution, ((1, 1), (1, 1), (0, 0)), mode="constant")) - (4.0 + reaction_rate) * solution
    return solution, remaining
```

```python
import functools

import jax
import jax.numpy as jnp
import numpy as np
from jax import lax
from jax.experimental import pallas as pl
from jax.experimental.pallas import tpu as pltpu
from jax.sharding import PartitionSpec as P

BEFORE = 3
INNER = 13
LANES = 128
GROUPS = 2
DEPTHS = (5, 4, 4)
PAD = 5
WEIGHT = np.float32(0.8)
KEEP = np.float32(1.0) - WEIGHT
MESH = pl.DeviceIdType.MESH

OFFSETS = ((-1, 0), (1, 0), (0, -1), (0, 1), (-1, -1), (-1, 1), (1, -1), (1, 1))
OPPOSITE = (1, 0, 3, 2, 7, 6, 5, 4)


def kernel(
    height, width, load_hbm, start_hbm, mass_hbm, sol_hbm, rem_hbm,
    fine, load, mass, coef, column_out, column_in, coarse, coarse_load, coarse_coef,
    edge_out, edge_in, corner_out, corner_in, temp,
    load_sem, out_sem, fine_send, fine_recv, coarse_send, coarse_recv,
):
    h, w = height // 2, width // 2
    pitch, coarse_pitch = width + 8, w + 16
    cells = height * width
    part = min(32, width)
    band, lane = lax.axis_index("band"), lax.axis_index("lane")
    bands, lanes = lax.axis_size("band"), lax.axis_size("lane")
    inside = {-1: (band > 0, lane > 0), 1: (band < bands - 1, lane < lanes - 1)}
    has = []
    for dy, dx in OFFSETS:
        if dx == 0:
            has.append(inside[dy][0])
        elif dy == 0:
            has.append(inside[dx][1])
        else:
            has.append(jnp.logical_and(inside[dy][0], inside[dx][1]))

    def neighbour(side):
        dy, dx = OFFSETS[side]
        return (band + dy, lane + dx)

    def at(y):
        return (y + 1) * pitch + 8

    def coarse_at(y):
        return (y + PAD) * coarse_pitch + 8

    def group_lanes(g):
        return pl.ds(g * LANES, LANES)

    def start_inputs():
        for g in range(GROUPS):
            target = fine.at[g, 0]

            @pl.loop(0, height)
            def _(y):
                pltpu.make_async_copy(
                    start_hbm.at[pl.ds(pl.multiple_of(y * width, 8), width), group_lanes(g)],
                    target.at[pl.ds(pl.multiple_of(at(y), 8), width), :],
                    load_sem.at[0, g],
                ).start()

        for g in range(GROUPS):
            pltpu.make_async_copy(mass_hbm.at[:, group_lanes(g)], mass.at[g], load_sem.at[1, g]).start()
            pltpu.make_async_copy(load_hbm.at[:, group_lanes(g)], load.at[g], load_sem.at[2, g]).start()

    def wait_input(which, g):
        source, target = ((start_hbm, coef), (mass_hbm, mass), (load_hbm, load))[which]
        pltpu.make_async_copy(source.at[:, group_lanes(g)], target.at[g], load_sem.at[which, g]).wait()

    def clear():
        zero8 = jnp.zeros((8, LANES), jnp.float32)
        for g in range(GROUPS):
            for b in range(2):
                ref = fine.at[g, b]
                ref[pl.ds(0, pitch), :] = jnp.zeros((pitch, LANES), jnp.float32)
                ref[pl.ds((height + 1) * pitch, pitch + 8), :] = jnp.zeros((pitch + 8, LANES), jnp.float32)

                @pl.loop(0, height // 8)
                def _(i):
                    for r in range(8):
                        ref[pl.ds(pl.multiple_of((i * 8 + r + 1) * pitch, 8), 8), :] = zero8

            rows = (h + 2 * PAD) * coarse_pitch // (h + 2 * PAD)

            @pl.loop(0, h + 2 * PAD)
            def _(y):
                for ref in (coarse.at[g, 1], coarse_load.at[g], coarse_coef.at[g]):
                    ref[pl.ds(pl.multiple_of(y * rows, 8), rows), :] = jnp.zeros((rows, LANES), jnp.float32)

    def enter():
        barrier = pltpu.get_barrier_semaphore()
        count = jnp.int32(0)
        for side in range(8):
            count = count + has[side].astype(jnp.int32)

            @pl.when(has[side])
            def _():
                pl.semaphore_signal(barrier, inc=1, device_id=neighbour(side), device_id_type=MESH)

        pl.semaphore_wait(barrier, count)

    def fine_copy(g, b, side):
        if side < 2:
            source = fine.at[g, b, pl.ds(at(0) if side == 0 else at(height - 1), width), :]
            target = fine.at[g, b, pl.ds(at(height) if side == 0 else at(-1), width), :]
        else:
            source = column_out.at[g, b, side - 2]
            target = column_in.at[g, b, OPPOSITE[side] - 2]
        return pltpu.make_async_remote_copy(
            src_ref=source, dst_ref=target,
            send_sem=fine_send.at[g, b, side], recv_sem=fine_recv.at[g, b, OPPOSITE[side]],
            device_id=neighbour(side), device_id_type=MESH,
        )

    def fine_arrival(g, b, side):
        if side < 2:
            target = fine.at[g, b, pl.ds(at(-1) if side == 0 else at(height), width), :]
        else:
            target = column_in.at[g, b, side - 2]
        return pltpu.make_async_remote_copy(
            src_ref=target, dst_ref=target,
            send_sem=fine_send.at[g, b, OPPOSITE[side]], recv_sem=fine_recv.at[g, b, side],
            device_id=neighbour(side), device_id_type=MESH,
        )

    def send_fine(g, b):
        ref = fine.at[g, b]
        for side, x in ((2, 0), (3, width - 1)):
            out = column_out.at[g, b, side - 2]
            for i in range(height // 8):
                out[pl.ds(8 * i, 8), :] = ref[pl.ds(at(8 * i) + x, 8, stride=pitch), :]
        for side in range(4):
            pl.when(has[side])(lambda side=side: fine_copy(g, b, side).start())

    def sent_fine(g, b):
        for side in range(4):
            pl.when(has[side])(lambda side=side: fine_copy(g, b, side).wait_send())

    def receive_fine(g, b):
        ref = fine.at[g, b]
        for side in range(4):
            pl.when(has[side])(lambda side=side: fine_arrival(g, b, side).wait_recv())
        for side, x in ((2, -1), (3, width)):

            @pl.when(has[side])
            def _():
                column = column_in.at[g, b, side - 2]
                for i in range(height // 8):
                    ref[pl.ds(at(8 * i) + x, 8, stride=pitch), :] = column[pl.ds(8 * i, 8), :]

    def fine_loop(g, b, finish, rows=8):
        ref = fine.at[g, b]

        @pl.loop(0, height // rows)
        def _(i):
            top = i * rows
            for p in range(width // part):
                centre = [
                    ref[pl.ds(pl.multiple_of(at(top + r - 1) + p * part, 8), part), :]
                    for r in range(rows + 2)
                ]
                for r in range(rows):
                    here = at(top + r) + p * part
                    around = (centre[r] + centre[r + 2]) + (
                        ref[pl.ds(here - 1, part), :] + ref[pl.ds(here + 1, part), :]
                    )
                    flat = pl.multiple_of((top + r) * width + p * part, 8)
                    finish(top, r, p, pl.multiple_of(here, 8), flat, centre[r + 1], around)

    def sweep_fine(g, b):
        out = fine.at[g, 1 - b]

        def finish(top, r, p, here, flat, centre, around):
            total = load[g, pl.ds(flat, part), :] + around
            out[pl.ds(here, part), :] = KEEP * centre + coef[g, pl.ds(flat, part), :] * total

        fine_loop(g, b, finish)

    def defect(g, flat, centre, around):
        return (load[g, pl.ds(flat, part), :] + around) - (4.0 + mass[g, pl.ds(flat, part), :]) * centre

    def halve(ref, slot, pair):
        scratch = ref.at[slot]
        scratch[...] = pair
        return scratch[pl.ds(0, part // 2, stride=2), :] + scratch[pl.ds(1, part // 2, stride=2), :]

    def coarsen_mass(g):
        rows = 4

        @pl.loop(0, height // rows)
        def _(i):
            for p in range(width // part):
                for r in range(0, rows, 2):
                    pair = []
                    for s in range(2):
                        flat = pl.multiple_of((i * rows + r + s) * width + p * part, 8)
                        here = mass[g, pl.ds(flat, part), :]
                        coef[g, pl.ds(flat, part), :] = WEIGHT / (4.0 + here)
                        pair.append(here)
                    summed = 0.5 * halve(temp, p * (rows // 2) + r // 2, pair[0] + pair[1])
                    place = coarse_at(i * (rows // 2) + r // 2) + p * (part // 2)
                    coarse_coef[g, pl.ds(pl.multiple_of(place, 8), part // 2), :] = WEIGHT / (4.0 + summed)

    def coarsen_defect(g, b):
        held = {}

        def finish(top, r, p, here, flat, centre, around):
            value = defect(g, flat, centre, around)
            if r % 2 == 0:
                held[p] = value
            else:
                summed = 0.5 * halve(temp, p * 4 + r // 2, held[p] + value)
                place = coarse_at(top // 2 + r // 2) + p * (part // 2)
                coarse_load[g, pl.ds(pl.multiple_of(place, 8), part // 2), :] = summed

        fine_loop(g, b, finish)

    def remain(g, b):
        def finish(top, r, p, here, flat, centre, around):
            coef[g, pl.ds(flat, part), :] = defect(g, flat, centre, around)

        fine_loop(g, b, finish)

    def blocks(side, depth):
        corner = depth - 1
        dy, dx = OFFSETS[side]
        if dx == 0:
            return (depth, w, 0 if dy < 0 else h - depth, 0, -depth if dy < 0 else h, 0)
        if dy == 0:
            return (h, depth, 0, 0 if dx < 0 else w - depth, 0, -depth if dx < 0 else w)
        return (
            corner, corner, 0 if dy < 0 else h - corner, 0 if dx < 0 else w - corner,
            -corner if dy < 0 else h, -corner if dx < 0 else w,
        )

    def buffers(g, e, side, depth):
        rows, columns = blocks(side, depth)[:2]
        if side < 4:
            return (
                edge_out.at[g, e, side, pl.ds(0, rows * columns), :],
                edge_in.at[g, e, side, pl.ds(0, rows * columns), :],
                edge_in.at[g, e, OPPOSITE[side], pl.ds(0, rows * columns), :],
            )
        return (
            corner_out.at[g, e, side - 4, pl.ds(0, rows * columns), :],
            corner_in.at[g, e, side - 4, pl.ds(0, rows * columns), :],
            corner_in.at[g, e, OPPOSITE[side] - 4, pl.ds(0, rows * columns), :],
        )

    def move(rows, columns, source, source_at, target, target_at):
        step = 8
        if rows % step == 0:

            @pl.loop(0, rows // step)
            def _(i):
                for r in range(step):
                    y = i * step + r
                    target[pl.ds(target_at(y), columns), :] = source[pl.ds(source_at(y), columns), :]
        else:
            for y in range(rows):
                target[pl.ds(target_at(y), columns), :] = source[pl.ds(source_at(y), columns), :]

    def sides_of(depth):
        return range(8 if depth > 1 else 4)

    def coarse_copy(g, e, side, depth):
        out, _, there = buffers(g, e, side, depth)
        return pltpu.make_async_remote_copy(
            src_ref=out, dst_ref=there,
            send_sem=coarse_send.at[g, e, side], recv_sem=coarse_recv.at[g, e, OPPOSITE[side]],
            device_id=neighbour(side), device_id_type=MESH,
        )

    def coarse_arrival(g, e, side, depth):
        _, here, _ = buffers(g, e, side, depth)
        return pltpu.make_async_remote_copy(
            src_ref=here, dst_ref=here,
            send_sem=coarse_send.at[g, e, OPPOSITE[side]], recv_sem=coarse_recv.at[g, e, side],
            device_id=neighbour(side), device_id_type=MESH,
        )

    def send_coarse(g, e, depth, ref):
        for side in sides_of(depth):
            rows, columns, y0, x0, _, _ = blocks(side, depth)
            out = edge_out.at[g, e, side] if side < 4 else corner_out.at[g, e, side - 4]
            move(rows, columns, ref, lambda y: coarse_at(y0 + y) + x0, out, lambda y: y * columns)
        for side in sides_of(depth):
            pl.when(has[side])(lambda side=side: coarse_copy(g, e, side, depth).start())

    def receive_coarse(g, e, depth, ref):
        for side in sides_of(depth):

            @pl.when(has[side])
            def _():
                coarse_arrival(g, e, side, depth).wait_recv()
                rows, columns, _, _, y1, x1 = blocks(side, depth)
                held = edge_in.at[g, e, side] if side < 4 else corner_in.at[g, e, side - 4]
                move(rows, columns, held, lambda y: y * columns, ref, lambda y: coarse_at(y1 + y) + x1)

    def sent_coarse(g, e, depth):
        for side in sides_of(depth):
            pl.when(has[side])(lambda side=side: coarse_copy(g, e, side, depth).wait_send())

    def first_coarse(g):
        out = coarse.at[g, 0]

        @pl.loop(0, h + 2 * PAD)
        def _(y):
            here = pl.ds(pl.multiple_of(y * coarse_pitch, 8), coarse_pitch)
            out[here, :] = coarse_coef[g, here, :] * coarse_load[g, here, :]

    def sweep_coarse(g, b, valid):
        ref, out = coarse.at[g, b], coarse.at[g, 1 - b]
        rim = (valid + 1) // 2 * 2
        span, left = (w + 8, -4) if valid else (w, 0)
        rows = 4

        @pl.loop(0, (h + 2 * rim) // rows)
        def _(i):
            top = i * rows - rim
            centre = [ref[pl.ds(coarse_at(top + r - 1) + left, span), :] for r in range(rows + 2)]
            for r in range(rows):
                here = coarse_at(top + r) + left
                around = (centre[r] + centre[r + 2]) + (
                    ref[pl.ds(here - 1, span), :] + ref[pl.ds(here + 1, span), :]
                )
                total = coarse_load[g, pl.ds(here, span), :] + around
                out[pl.ds(here, span), :] = KEEP * centre[r + 1] + coarse_coef[g, pl.ds(here, span), :] * total

    def correct(g, b, c):
        ref, values = fine.at[g, b], coarse.at[g, c]

        def spread(slot, value):
            scratch = temp.at[slot]
            scratch[pl.ds(0, part // 2, stride=2), :] = value
            scratch[pl.ds(1, part // 2, stride=2), :] = value
            return scratch[...]

        def add(y, wide, p):
            here = pl.ds(pl.multiple_of(at(y) + p * part, 8), part)
            ref[here, :] = ref[here, :] + wide

        rows = 4

        @pl.loop(0, h // rows)
        def _(i):
            for r in range(rows):
                for p in range(width // part):
                    place = coarse_at(i * rows + r) + p * (part // 2)
                    wide = spread(r * 2 + p, values[pl.ds(pl.multiple_of(place, 8), part // 2), :])
                    for s in range(2):
                        add((i * rows + r) * 2 + s, wide, p)

        for side, y in ((0, -1), (1, height)):
            for p in range(width // part):
                place = coarse_at(-1 if y < 0 else h) + p * (part // 2)
                add(y, spread(side * 2 + p, values[pl.ds(place, part // 2), :]), p)
        for side, x in ((2, -1), (3, width)):
            for p in range(height // part):
                place = coarse_at(p * (part // 2)) + (-1 if x < 0 else w)
                wide = spread(side * 2 + p, values[pl.ds(place, part // 2, stride=coarse_pitch), :])
                for i in range(part // 8):
                    here = pl.ds(at(p * part + 8 * i) + x, 8, stride=pitch)
                    ref[here, :] = ref[here, :] + wide[8 * i : 8 * i + 8]

    def write_solution(g, b):
        ref = fine.at[g, b]

        @pl.loop(0, height)
        def _(y):
            pltpu.make_async_copy(
                ref.at[pl.ds(pl.multiple_of(at(y), 8), width), :],
                sol_hbm.at[pl.ds(pl.multiple_of(y * width, 8), width), group_lanes(g)],
                out_sem.at[0, g],
            ).start()

    def remaining_copy(g):
        return pltpu.make_async_copy(coef.at[g], rem_hbm.at[:, group_lanes(g)], out_sem.at[1, g])

    both = range(GROUPS)
    start_inputs()
    clear()
    enter()
    for g in both:
        wait_input(0, g)
        send_fine(g, 0)
    for g in both:
        wait_input(1, g)
        coarsen_mass(g)
        wait_input(2, g)
    now = 0
    for sweep in range(BEFORE):
        for g in both:
            receive_fine(g, now)
            if sweep >= 1:
                sent_fine(g, 1 - now)
            sweep_fine(g, now)
            send_fine(g, 1 - now)
            if sweep < GROUPS:
                send_coarse(sweep, 0, DEPTHS[0], coarse_coef.at[sweep]) if g == GROUPS - 1 else None
        now = 1 - now
    for g in both:
        receive_fine(g, now)
        coarsen_defect(g, now)
        send_coarse(g, 1, DEPTHS[0], coarse_load.at[g])
    for g in both:
        receive_coarse(g, 0, DEPTHS[0], coarse_coef.at[g])
    inner, valid, c = 1, DEPTHS[0], 0
    for e, depth in enumerate(DEPTHS):
        last = e == len(DEPTHS) - 1
        count = depth - 1 if last else depth
        for g in both:
            b = c
            if e == 0:
                receive_coarse(g, 1, depth, coarse_load.at[g])
                first_coarse(g)
            else:
                receive_coarse(g, 1 + e, depth, coarse.at[g, b])
            for i in range(count):
                sweep_coarse(g, b, depth - 1 - i)
                b = 1 - b
            if not last:
                send_coarse(g, 2 + e, DEPTHS[e + 1], coarse.at[g, b])
            else:
                sent_fine(g, now)
                correct(g, now, b)
                sent_fine(g, 1 - now)
                sweep_fine(g, now)
                send_fine(g, 1 - now)
        c = (c + count) % 2
        inner += count
    assert inner == INNER
    now = 1 - now
    for g in both:
        receive_fine(g, now)
        sweep_fine(g, now)
        send_fine(g, 1 - now)
        write_solution(g, 1 - now)
    now = 1 - now
    for g in both:
        receive_fine(g, now)
        remain(g, now)
        remaining_copy(g).start()
    for g in both:
        for b in range(2):
            sent_fine(g, b)
        for e in range(len(DEPTHS) + 1):
            sent_coarse(g, e, DEPTHS[max(e - 1, 0)])
        pltpu.make_async_copy(coef.at[g], sol_hbm.at[:, group_lanes(g)], out_sem.at[0, g]).wait()
        remaining_copy(g).wait()


def body(load_terms, start_values, reaction_rate):
    height, width, layers = load_terms.shape
    h, w = height // 2, width // 2
    flat = (height * width, layers)
    fine_rows = (height + 2) * (width + 8) + 8
    coarse_rows = (h + 2 * PAD) * (w + 16)
    exchanges = len(DEPTHS) + 1
    edge = max(DEPTHS) * max(h, w)
    corner = -(-((max(DEPTHS) - 1) ** 2) // 8) * 8
    f32 = jnp.float32
    any_space = pl.BlockSpec(memory_space=pl.ANY)
    results = pl.pallas_call(
        functools.partial(kernel, height, width),
        out_shape=[jax.ShapeDtypeStruct(flat, f32)] * 2,
        in_specs=[any_space] * 3,
        out_specs=[any_space] * 2,
        scratch_shapes=[
            pltpu.VMEM((GROUPS, 2, fine_rows, LANES), f32),
            pltpu.VMEM((GROUPS, height * width, LANES), f32),
            pltpu.VMEM((GROUPS, height * width, LANES), f32),
            pltpu.VMEM((GROUPS, height * width, LANES), f32),
            pltpu.VMEM((GROUPS, 2, 2, height, LANES), f32),
            pltpu.VMEM((GROUPS, 2, 2, height, LANES), f32),
            pltpu.VMEM((GROUPS, 2, coarse_rows, LANES), f32),
            pltpu.VMEM((GROUPS, coarse_rows, LANES), f32),
            pltpu.VMEM((GROUPS, coarse_rows, LANES), f32),
            pltpu.VMEM((GROUPS, exchanges, 4, edge, LANES), f32),
            pltpu.VMEM((GROUPS, exchanges, 4, edge, LANES), f32),
            pltpu.VMEM((GROUPS, exchanges, 4, corner, LANES), f32),
            pltpu.VMEM((GROUPS, exchanges, 4, corner, LANES), f32),
            pltpu.VMEM((8, min(32, width), LANES), f32),
            pltpu.SemaphoreType.DMA((3, GROUPS)),
            pltpu.SemaphoreType.DMA((2, GROUPS)),
            pltpu.SemaphoreType.DMA((GROUPS, 2, 4)),
            pltpu.SemaphoreType.DMA((GROUPS, 2, 4)),
            pltpu.SemaphoreType.DMA((GROUPS, exchanges, 8)),
            pltpu.SemaphoreType.DMA((GROUPS, exchanges, 8)),
        ],
        compiler_params=pltpu.CompilerParams(
            collective_id=0, has_side_effects=True, vmem_limit_bytes=50 * 1024 * 1024
        ),
    )(load_terms.reshape(flat), start_values.reshape(flat), reaction_rate.reshape(flat))
    return tuple(result.reshape(height, width, layers) for result in results)


def solution(mesh):
    spec = P("band", "lane", None)
    return jax.shard_map(
        body, mesh=mesh, in_specs=(spec, spec, spec), out_specs=(spec, spec), check_vma=False
    )
```

```python
import functools

import jax
import jax.numpy as jnp
import numpy as np
from jax import lax
from jax.experimental import pallas as pl
from jax.experimental.pallas import tpu as pltpu
from jax.sharding import PartitionSpec as P

BEFORE = 3
INNER = 13
LANES = 128
GROUPS = 2
DEPTHS = (3, 3, 3, 4)
PAD = 5
WEIGHT = np.float32(0.8)
KEEP = np.float32(1.0) - WEIGHT
MESH = pl.DeviceIdType.MESH

OFFSETS = ((-1, 0), (1, 0), (0, -1), (0, 1), (-1, -1), (-1, 1), (1, -1), (1, 1))
OPPOSITE = (1, 0, 3, 2, 7, 6, 5, 4)


def kernel(
    height, width, load_hbm, start_hbm, mass_hbm, final, load, mass,
    fine, coef, row_in, column_out, column_in, coarse, coarse_load, coarse_coef,
    edge_out, edge_in, corner_out, corner_in, temp,
    load_sem, fine_send, fine_recv, coarse_send, coarse_recv,
):
    h, w = height // 2, width // 2
    pitch, coarse_pitch = width + 8, w + 16
    cells = height * width
    part = min(32, width)
    band, lane = lax.axis_index("band"), lax.axis_index("lane")
    bands, lanes = lax.axis_size("band"), lax.axis_size("lane")
    inside = {-1: (band > 0, lane > 0), 1: (band < bands - 1, lane < lanes - 1)}
    has = []
    for dy, dx in OFFSETS:
        if dx == 0:
            has.append(inside[dy][0])
        elif dy == 0:
            has.append(inside[dx][1])
        else:
            has.append(jnp.logical_and(inside[dy][0], inside[dx][1]))

    def neighbour(side):
        dy, dx = OFFSETS[side]
        return (band + dy, lane + dx)

    def at(y):
        return (y + 1) * pitch + 8

    def coarse_at(y):
        return (y + PAD) * coarse_pitch + 8

    def group_lanes(g):
        return pl.ds(g * LANES, LANES)

    def start_values(g):
        target = fine.at[g, 0]

        @pl.loop(0, height)
        def _(y):
            pltpu.make_async_copy(
                start_hbm.at[pl.ds(pl.multiple_of(y * width, 8), width), group_lanes(g)],
                target.at[pl.ds(pl.multiple_of(at(y), 8), width), :],
                load_sem.at[0, g],
            ).start()

    def start_terms(g):
        pltpu.make_async_copy(mass_hbm.at[:, group_lanes(g)], mass.at[g], load_sem.at[1, g]).start()
        pltpu.make_async_copy(load_hbm.at[:, group_lanes(g)], load.at[g], load_sem.at[2, g]).start()

    def wait_input(which, g):
        source, target = ((start_hbm, coef), (mass_hbm, mass), (load_hbm, load))[which]
        pltpu.make_async_copy(source.at[:, group_lanes(g)], target.at[g], load_sem.at[which, g]).wait()

    def clear_rows():
        for g in range(GROUPS):
            for b in range(2):
                fine[g, b, pl.ds(at(-1), width), :] = jnp.zeros((width, LANES), jnp.float32)
                fine[g, b, pl.ds(at(height), width), :] = jnp.zeros((width, LANES), jnp.float32)

    def clear_rest(g):
        zero8 = jnp.zeros((8, LANES), jnp.float32)
        step = 8

        @pl.loop(0, height // step)
        def _(i):
            for r in range(step):
                here = pl.ds(pl.multiple_of((i * step + r + 1) * pitch, 8), 8)
                fine[g, 0, here, :] = zero8
                fine[g, 1, here, :] = zero8
                final[g, here, :] = zero8

        for ref in (fine.at[g, 0], fine.at[g, 1], final.at[g]):
            for y in (0, height + 1, height + 2):
                ref[pl.ds(y * pitch, 8), :] = zero8
        for y in (-1, height):
            final[g, pl.ds(at(y), width), :] = jnp.zeros((width, LANES), jnp.float32)

        @pl.loop(0, h + 2 * PAD)
        def _(y):
            here = pl.ds(pl.multiple_of(y * coarse_pitch, 8), coarse_pitch)
            for ref in (coarse.at[g, 1], coarse_load.at[g], coarse_coef.at[g]):
                ref[here, :] = jnp.zeros((coarse_pitch, LANES), jnp.float32)

    def enter():
        barrier = pltpu.get_barrier_semaphore()
        count = jnp.int32(0)
        for side in range(8):
            count = count + has[side].astype(jnp.int32)

            @pl.when(has[side])
            def _():
                pl.semaphore_signal(barrier, inc=1, device_id=neighbour(side), device_id_type=MESH)

        pl.semaphore_wait(barrier, count)

    def fine_place(g, b, side, arrives):
        if side >= 2:
            return (column_in if arrives else column_out).at[g, min(b, 1), side - 2]
        if b == 2:
            if arrives:
                return row_in.at[g, side]
            return final.at[g, pl.ds(at(0) if side == 0 else at(height - 1), width), :]
        inner, outer = (0, -1) if side == 0 else (height - 1, height)
        return fine.at[g, b, pl.ds(at(outer if arrives else inner), width), :]

    def fine_copy(g, b, side):
        return pltpu.make_async_remote_copy(
            src_ref=fine_place(g, b, side, False), dst_ref=fine_place(g, b, OPPOSITE[side], True),
            send_sem=fine_send.at[g, min(b, 1), side], recv_sem=fine_recv.at[g, min(b, 1), OPPOSITE[side]],
            device_id=neighbour(side), device_id_type=MESH,
        )

    def fine_arrival(g, b, side):
        place = fine_place(g, b, side, True)
        return pltpu.make_async_remote_copy(
            src_ref=place, dst_ref=place,
            send_sem=fine_send.at[g, min(b, 1), OPPOSITE[side]], recv_sem=fine_recv.at[g, min(b, 1), side],
            device_id=neighbour(side), device_id_type=MESH,
        )

    def values_of(g, b):
        return final.at[g] if b == 2 else fine.at[g, b]

    def send_rows(g, b):
        for side in (0, 1):
            pl.when(has[side])(lambda side=side: fine_copy(g, b, side).start())

    def send_columns(g, b):
        ref = values_of(g, b)
        for side, x in ((2, 0), (3, width - 1)):
            out = column_out.at[g, min(b, 1), side - 2]
            for i in range(height // 8):
                out[pl.ds(8 * i, 8), :] = ref[pl.ds(at(8 * i) + x, 8, stride=pitch), :]
        for side in (2, 3):
            pl.when(has[side])(lambda side=side: fine_copy(g, b, side).start())

    def sent_fine(g, b):
        for side in range(4):
            pl.when(has[side])(lambda side=side: fine_copy(g, b, side).wait_send())

    def receive_fine(g, b):
        ref = values_of(g, b)
        for side in (2, 3, 0, 1):
            pl.when(has[side])(lambda side=side: fine_arrival(g, b, side).wait_recv())
        for side, x in ((2, -1), (3, width)):

            @pl.when(has[side])
            def _():
                column = column_in.at[g, min(b, 1), side - 2]
                for i in range(height // 8):
                    ref[pl.ds(at(8 * i) + x, 8, stride=pitch), :] = column[pl.ds(8 * i, 8), :]

    rows = 8
    chunks = height // rows

    def fine_chunk(g, b, i, finish):
        ref = fine.at[g, b]
        top = i * rows
        for p in range(width // part):
            centre = [
                ref[pl.ds(pl.multiple_of(at(top + r - 1) + p * part, 8), part), :]
                for r in range(rows + 2)
            ]
            for r in range(rows):
                here = at(top + r) + p * part
                around = (centre[r] + centre[r + 2]) + (
                    ref[pl.ds(here - 1, part), :] + ref[pl.ds(here + 1, part), :]
                )
                flat = pl.multiple_of((top + r) * width + p * part, 8)
                finish(top, r, p, pl.multiple_of(here, 8), flat, centre[r + 1], around)

    def fine_loop(g, b, finish, between):
        @pl.loop(0, 2)
        def _(i):
            fine_chunk(g, b, i * (chunks - 1), finish)

        between()

        @pl.loop(1, chunks - 1)
        def _(i):
            fine_chunk(g, b, i, finish)

    def sweep_fine(g, b, new):
        out = values_of(g, new)

        def finish(top, r, p, here, flat, centre, around):
            total = load[g, pl.ds(flat, part), :] + around
            out[pl.ds(here, part), :] = KEEP * centre + coef[g, pl.ds(flat, part), :] * total

        fine_loop(g, b, finish, lambda: send_rows(g, new))
        send_columns(g, new)

    def defect(g, flat, centre, around):
        return (load[g, pl.ds(flat, part), :] + around) - (4.0 + mass[g, pl.ds(flat, part), :]) * centre

    def halve(ref, slot, pair):
        scratch = ref.at[slot]
        scratch[...] = pair
        return scratch[pl.ds(0, part // 2, stride=2), :] + scratch[pl.ds(1, part // 2, stride=2), :]

    def coarsen_mass(g):
        step = 4

        @pl.loop(0, height // step)
        def _(i):
            for p in range(width // part):
                for r in range(0, step, 2):
                    pair = []
                    for s in range(2):
                        flat = pl.multiple_of((i * step + r + s) * width + p * part, 8)
                        here = mass[g, pl.ds(flat, part), :]
                        coef[g, pl.ds(flat, part), :] = WEIGHT / (4.0 + here)
                        pair.append(here)
                    summed = 0.5 * halve(temp, p * (step // 2) + r // 2, pair[0] + pair[1])
                    place = coarse_at(i * (step // 2) + r // 2) + p * (part // 2)
                    coarse_coef[g, pl.ds(pl.multiple_of(place, 8), part // 2), :] = WEIGHT / (4.0 + summed)

    def coarsen_defect(g, b):
        held = {}

        def finish(top, r, p, here, flat, centre, around):
            value = defect(g, flat, centre, around)
            if r % 2 == 0:
                held[p] = value
            else:
                summed = 0.5 * halve(temp, p * 4 + r // 2, held[p] + value)
                place = coarse_at(top // 2 + r // 2) + p * (part // 2)
                coarse_load[g, pl.ds(pl.multiple_of(place, 8), part // 2), :] = summed

        fine_loop(g, b, finish, lambda: send_coarse(g, 1, DEPTHS[0], coarse_load.at[g], (0, 1)))
        send_coarse(g, 1, DEPTHS[0], coarse_load.at[g], (2, 3, 4, 5, 6, 7))

    def blocks(side, depth):
        corner = depth - 1
        dy, dx = OFFSETS[side]
        if dx == 0:
            return (depth, w, 0 if dy < 0 else h - depth, 0, -depth if dy < 0 else h, 0)
        if dy == 0:
            return (h, depth, 0, 0 if dx < 0 else w - depth, 0, -depth if dx < 0 else w)
        return (
            corner, corner, 0 if dy < 0 else h - corner, 0 if dx < 0 else w - corner,
            -corner if dy < 0 else h, -corner if dx < 0 else w,
        )

    def buffers(g, e, side, depth):
        rows, columns = blocks(side, depth)[:2]
        if side < 4:
            return (
                edge_out.at[g, e, side, pl.ds(0, rows * columns), :],
                edge_in.at[g, e, side, pl.ds(0, rows * columns), :],
                edge_in.at[g, e, OPPOSITE[side], pl.ds(0, rows * columns), :],
            )
        return (
            corner_out.at[g, e, side - 4, pl.ds(0, rows * columns), :],
            corner_in.at[g, e, side - 4, pl.ds(0, rows * columns), :],
            corner_in.at[g, e, OPPOSITE[side] - 4, pl.ds(0, rows * columns), :],
        )

    def move(rows, columns, source, source_at, target, target_at):
        step = 8
        if rows % step == 0:

            @pl.loop(0, rows // step)
            def _(i):
                for r in range(step):
                    y = i * step + r
                    target[pl.ds(target_at(y), columns), :] = source[pl.ds(source_at(y), columns), :]
        else:
            for y in range(rows):
                target[pl.ds(target_at(y), columns), :] = source[pl.ds(source_at(y), columns), :]

    def sides_of(depth):
        return range(8 if depth > 1 else 4)

    def coarse_copy(g, e, side, depth):
        out, _, there = buffers(g, e, side, depth)
        return pltpu.make_async_remote_copy(
            src_ref=out, dst_ref=there,
            send_sem=coarse_send.at[g, e, side], recv_sem=coarse_recv.at[g, e, OPPOSITE[side]],
            device_id=neighbour(side), device_id_type=MESH,
        )

    def coarse_arrival(g, e, side, depth):
        _, here, _ = buffers(g, e, side, depth)
        return pltpu.make_async_remote_copy(
            src_ref=here, dst_ref=here,
            send_sem=coarse_send.at[g, e, OPPOSITE[side]], recv_sem=coarse_recv.at[g, e, side],
            device_id=neighbour(side), device_id_type=MESH,
        )

    def send_coarse(g, e, depth, ref, sides=(4, 5, 6, 7, 0, 1, 2, 3)):
        sides = [side for side in sides if side in sides_of(depth)]
        for side in sides:
            rows, columns, y0, x0, _, _ = blocks(side, depth)
            out = edge_out.at[g, e, side] if side < 4 else corner_out.at[g, e, side - 4]
            move(rows, columns, ref, lambda y: coarse_at(y0 + y) + x0, out, lambda y: y * columns)
        for side in sides:
            pl.when(has[side])(lambda side=side: coarse_copy(g, e, side, depth).start())

    def receive_coarse(g, e, depth, ref):
        for side in sides_of(depth):

            @pl.when(has[side])
            def _():
                coarse_arrival(g, e, side, depth).wait_recv()
                rows, columns, _, _, y1, x1 = blocks(side, depth)
                held = edge_in.at[g, e, side] if side < 4 else corner_in.at[g, e, side - 4]
                move(rows, columns, held, lambda y: y * columns, ref, lambda y: coarse_at(y1 + y) + x1)

    def sent_coarse(g, e, depth):
        for side in sides_of(depth):
            pl.when(has[side])(lambda side=side: coarse_copy(g, e, side, depth).wait_send())

    def first_coarse(g):
        out = coarse.at[g, 0]

        @pl.loop(0, h + 2 * PAD)
        def _(y):
            here = pl.ds(pl.multiple_of(y * coarse_pitch, 8), coarse_pitch)
            out[here, :] = coarse_coef[g, here, :] * coarse_load[g, here, :]

    def sweep_coarse(g, b, valid):
        ref, out = coarse.at[g, b], coarse.at[g, 1 - b]
        rim = (valid + 1) // 2 * 2
        span, left = (w + 8, -4) if valid else (w, 0)
        rows = 4

        @pl.loop(0, (h + 2 * rim) // rows)
        def _(i):
            top = i * rows - rim
            centre = [ref[pl.ds(coarse_at(top + r - 1) + left, span), :] for r in range(rows + 2)]
            for r in range(rows):
                here = coarse_at(top + r) + left
                around = (centre[r] + centre[r + 2]) + (
                    ref[pl.ds(here - 1, span), :] + ref[pl.ds(here + 1, span), :]
                )
                total = coarse_load[g, pl.ds(here, span), :] + around
                out[pl.ds(here, span), :] = KEEP * centre[r + 1] + coarse_coef[g, pl.ds(here, span), :] * total

    def correct(g, b, c):
        ref, values = fine.at[g, b], coarse.at[g, c]

        def spread(slot, value):
            scratch = temp.at[slot]
            scratch[pl.ds(0, part // 2, stride=2), :] = value
            scratch[pl.ds(1, part // 2, stride=2), :] = value
            return scratch[...]

        def add(y, wide, p):
            here = pl.ds(pl.multiple_of(at(y) + p * part, 8), part)
            ref[here, :] = ref[here, :] + wide

        rows = 4

        @pl.loop(0, h // rows)
        def _(i):
            for r in range(rows):
                for p in range(width // part):
                    place = coarse_at(i * rows + r) + p * (part // 2)
                    wide = spread(r * 2 + p, values[pl.ds(pl.multiple_of(place, 8), part // 2), :])
                    for s in range(2):
                        add((i * rows + r) * 2 + s, wide, p)

        for side, y in ((0, -1), (1, height)):
            for p in range(width // part):
                place = coarse_at(-1 if y < 0 else h) + p * (part // 2)
                add(y, spread(side * 2 + p, values[pl.ds(place, part // 2), :]), p)
        for side, x in ((2, -1), (3, width)):
            for p in range(height // part):
                place = coarse_at(p * (part // 2)) + (-1 if x < 0 else w)
                wide = spread(side * 2 + p, values[pl.ds(place, part // 2, stride=coarse_pitch), :])
                for i in range(part // 8):
                    here = pl.ds(at(p * part + 8 * i) + x, 8, stride=pitch)
                    ref[here, :] = ref[here, :] + wide[8 * i : 8 * i + 8]

    both = range(GROUPS)
    start_values(0)
    clear_rows()
    start_values(1)
    for g in both:
        start_terms(g)
    enter()
    for g in both:
        wait_input(0, g)
        send_rows(g, 0)
        send_columns(g, 0)
    for g in both:
        clear_rest(g)
        wait_input(1, g)
        coarsen_mass(g)
        wait_input(2, g)
    parts = ((0, 1), (2, 4, 5), (3, 6, 7))
    now = 0
    for sweep in range(BEFORE):
        for g in both:
            receive_fine(g, now)
            if sweep >= 1:
                sent_fine(g, 1 - now)
            sweep_fine(g, now, 1 - now)
            send_coarse(g, 0, DEPTHS[0], coarse_coef.at[g], parts[sweep])
        now = 1 - now
    for g in both:
        receive_fine(g, now)
        coarsen_defect(g, now)
    for g in both:
        receive_coarse(g, 0, DEPTHS[0], coarse_coef.at[g])
    inner, c = 1, 0
    for e, depth in enumerate(DEPTHS):
        last = e == len(DEPTHS) - 1
        count = depth - 1 if last else depth
        for g in both:
            b = c
            if e == 0:
                receive_coarse(g, 1, depth, coarse_load.at[g])
                first_coarse(g)
            else:
                receive_coarse(g, 1 + e, depth, coarse.at[g, b])
            for i in range(count):
                sweep_coarse(g, b, depth - 1 - i)
                b = 1 - b
            if not last:
                send_coarse(g, 2 + e, DEPTHS[e + 1], coarse.at[g, b])
            else:
                sent_fine(g, now)
                correct(g, now, b)
                sent_fine(g, 1 - now)
                sweep_fine(g, now, 1 - now)
        c = (c + count) % 2
        inner += count
    assert inner == INNER and now == 1
    for g in both:
        receive_fine(g, 0)
        sweep_fine(g, 0, 2)
        for e in range(len(DEPTHS) + 1):
            sent_coarse(g, e, DEPTHS[max(e - 1, 0)])
    for g in both:
        receive_fine(g, 2)
        for side, y in ((0, -1), (1, height)):

            @pl.when(has[side])
            def _():
                final[g, pl.ds(at(y), width), :] = row_in[g, side]

        sent_fine(g, 0)
        sent_fine(g, 2)


def finish_kernel(height, width, final, load, mass, sol_hbm, rem_hbm, rem, sol_sem, rem_sem):
    pitch, part, rows = width + 8, min(32, width), 8
    chunks = 2 if height % (2 * rows) == 0 else 1
    span = height // chunks

    def group_lanes(g):
        return pl.ds(g * LANES, LANES)

    def at(y):
        return (y + 1) * pitch + 8

    def remaining_copy(g, c):
        here = pl.ds(c * span * width, span * width)
        return pltpu.make_async_copy(rem.at[g, here, :], rem_hbm.at[here, group_lanes(g)], rem_sem.at[g, c])

    for g in range(GROUPS):

        @pl.loop(0, height)
        def _(y):
            pltpu.make_async_copy(
                final.at[g, pl.ds(pl.multiple_of(at(y), 8), width), :],
                sol_hbm.at[pl.ds(pl.multiple_of(y * width, 8), width), group_lanes(g)],
                sol_sem.at[g],
            ).start()

        for c in range(chunks):

            @pl.loop(0, span // rows)
            def _(i):
                top = c * span + i * rows
                for p in range(width // part):
                    centre = [
                        final[g, pl.ds(pl.multiple_of(at(top + r - 1) + p * part, 8), part), :]
                        for r in range(rows + 2)
                    ]
                    for r in range(rows):
                        here = at(top + r) + p * part
                        around = (centre[r] + centre[r + 2]) + (
                            final[g, pl.ds(here - 1, part), :] + final[g, pl.ds(here + 1, part), :]
                        )
                        flat = pl.ds(pl.multiple_of((top + r) * width + p * part, 8), part)
                        rem[g, flat, :] = (load[g, flat, :] + around) - (4.0 + mass[g, flat, :]) * centre[r + 1]

            remaining_copy(g, c).start()
    for g in range(GROUPS):
        for c in range(chunks):
            remaining_copy(g, c).wait()
        pltpu.make_async_copy(rem.at[g], sol_hbm.at[:, group_lanes(g)], sol_sem.at[g]).wait()


def body(load_terms, start_values, reaction_rate):
    height, width, layers = load_terms.shape
    h, w = height // 2, width // 2
    flat = (height * width, layers)
    fine_rows = (height + 2) * (width + 8) + 8
    coarse_rows = (h + 2 * PAD) * (w + 16)
    exchanges = len(DEPTHS) + 1
    edge = max(DEPTHS) * max(h, w)
    corner = -(-((max(DEPTHS) - 1) ** 2) // 8) * 8
    f32 = jnp.float32
    any_space = pl.BlockSpec(memory_space=pl.ANY)
    vmem_space = pl.BlockSpec(memory_space=pltpu.VMEM)
    cells = height * width
    held = pl.pallas_call(
        functools.partial(kernel, height, width),
        out_shape=[
            pltpu.VMEM((GROUPS, fine_rows, LANES), f32),
            pltpu.VMEM((GROUPS, cells, LANES), f32),
            pltpu.VMEM((GROUPS, cells, LANES), f32),
        ],
        in_specs=[any_space] * 3,
        out_specs=[vmem_space] * 3,
        scratch_shapes=[
            pltpu.VMEM((GROUPS, 2, fine_rows, LANES), f32),
            pltpu.VMEM((GROUPS, cells, LANES), f32),
            pltpu.VMEM((GROUPS, 2, width, LANES), f32),
            pltpu.VMEM((GROUPS, 2, 2, height, LANES), f32),
            pltpu.VMEM((GROUPS, 2, 2, height, LANES), f32),
            pltpu.VMEM((GROUPS, 2, coarse_rows, LANES), f32),
            pltpu.VMEM((GROUPS, coarse_rows, LANES), f32),
            pltpu.VMEM((GROUPS, coarse_rows, LANES), f32),
            pltpu.VMEM((GROUPS, exchanges, 4, edge, LANES), f32),
            pltpu.VMEM((GROUPS, exchanges, 4, edge, LANES), f32),
            pltpu.VMEM((GROUPS, exchanges, 4, corner, LANES), f32),
            pltpu.VMEM((GROUPS, exchanges, 4, corner, LANES), f32),
            pltpu.VMEM((8, min(32, width), LANES), f32),
            pltpu.SemaphoreType.DMA((3, GROUPS)),
            pltpu.SemaphoreType.DMA((GROUPS, 2, 4)),
            pltpu.SemaphoreType.DMA((GROUPS, 2, 4)),
            pltpu.SemaphoreType.DMA((GROUPS, exchanges, 8)),
            pltpu.SemaphoreType.DMA((GROUPS, exchanges, 8)),
        ],
        compiler_params=pltpu.CompilerParams(
            collective_id=0, has_side_effects=True, vmem_limit_bytes=48 * 1024 * 1024
        ),
    )(load_terms.reshape(flat), start_values.reshape(flat), reaction_rate.reshape(flat))
    results = pl.pallas_call(
        functools.partial(finish_kernel, height, width),
        out_shape=[jax.ShapeDtypeStruct(flat, f32)] * 2,
        in_specs=[vmem_space] * 3,
        out_specs=[any_space] * 2,
        scratch_shapes=[
            pltpu.VMEM((GROUPS, cells, LANES), f32),
            pltpu.SemaphoreType.DMA((GROUPS,)),
            pltpu.SemaphoreType.DMA((GROUPS, 2)),
        ],
        compiler_params=pltpu.CompilerParams(vmem_limit_bytes=24 * 1024 * 1024),
    )(*held)
    return tuple(result.reshape(height, width, layers) for result in results)


def solution(mesh):
    spec = P("band", "lane", None)
    return jax.shard_map(
        body, mesh=mesh, in_specs=(spec, spec, spec), out_specs=(spec, spec), check_vma=False
    )
```

```python
import functools

import jax
import jax.numpy as jnp
import numpy as np
from jax import lax
from jax.experimental import pallas as pl
from jax.experimental.pallas import tpu as pltpu
from jax.sharding import PartitionSpec as P

BEFORE = 3
INNER = 13
LANES = 128
GROUPS = 2
DEPTHS = (2, 3, 3, 3, 2)
PARTS = ((), (0, 1), (2, 4, 5), (3, 6, 7))
PAD = 5
WEIGHT = np.float32(0.8)
KEEP = np.float32(1.0) - WEIGHT
MESH = pl.DeviceIdType.MESH

OFFSETS = ((-1, 0), (1, 0), (0, -1), (0, 1), (-1, -1), (-1, 1), (1, -1), (1, 1))
OPPOSITE = (1, 0, 3, 2, 7, 6, 5, 4)


def kernel(
    height, width, load_hbm, start_hbm, mass_hbm, final, load, mass,
    fine, coef, row_in, column_out, column_in, coarse, coarse_load, coarse_coef,
    edge_out, edge_in, corner_out, corner_in, temp,
    load_sem, fine_send, fine_recv, coarse_send, coarse_recv,
):
    h, w = height // 2, width // 2
    pitch, coarse_pitch = width + 8, w + 16
    cells = height * width
    part = min(32, width)
    band, lane = lax.axis_index("band"), lax.axis_index("lane")
    bands, lanes = lax.axis_size("band"), lax.axis_size("lane")
    inside = {-1: (band > 0, lane > 0), 1: (band < bands - 1, lane < lanes - 1)}
    has = []
    for dy, dx in OFFSETS:
        if dx == 0:
            has.append(inside[dy][0])
        elif dy == 0:
            has.append(inside[dx][1])
        else:
            has.append(jnp.logical_and(inside[dy][0], inside[dx][1]))

    def neighbour(side):
        dy, dx = OFFSETS[side]
        return (band + dy, lane + dx)

    def at(y):
        return (y + 1) * pitch + 8

    def coarse_at(y):
        return (y + PAD) * coarse_pitch + 8

    def group_lanes(g):
        return pl.ds(g * LANES, LANES)

    def start_values(g):
        target = fine.at[g, 0]

        @pl.loop(0, height)
        def _(y):
            pltpu.make_async_copy(
                start_hbm.at[pl.ds(pl.multiple_of(y * width, 8), width), group_lanes(g)],
                target.at[pl.ds(pl.multiple_of(at(y), 8), width), :],
                load_sem.at[0, g],
            ).start()

    def start_terms(g):
        pltpu.make_async_copy(mass_hbm.at[:, group_lanes(g)], mass.at[g], load_sem.at[1, g]).start()
        pltpu.make_async_copy(load_hbm.at[:, group_lanes(g)], load.at[g], load_sem.at[2, g]).start()

    def wait_input(which, g):
        source, target = ((start_hbm, coef), (mass_hbm, mass), (load_hbm, load))[which]
        pltpu.make_async_copy(source.at[:, group_lanes(g)], target.at[g], load_sem.at[which, g]).wait()

    def clear_rows():
        for side, y in ((0, -1), (1, height)):

            @pl.when(jnp.logical_not(has[side]))
            def _():
                for g in range(GROUPS):
                    for b in range(2):
                        fine[g, b, pl.ds(at(y), width), :] = jnp.zeros((width, LANES), jnp.float32)

    def clear_rest(g):
        zero8 = jnp.zeros((8, LANES), jnp.float32)
        step = 8

        @pl.loop(0, height // step)
        def _(i):
            for r in range(step):
                here = pl.ds(pl.multiple_of((i * step + r + 1) * pitch, 8), 8)
                fine[g, 0, here, :] = zero8
                fine[g, 1, here, :] = zero8
                final[g, here, :] = zero8

        for ref in (fine.at[g, 0], fine.at[g, 1], final.at[g]):
            for y in (0, height + 1, height + 2):
                ref[pl.ds(y * pitch, 8), :] = zero8
        for y in (-1, height):
            final[g, pl.ds(at(y), width), :] = jnp.zeros((width, LANES), jnp.float32)

        @pl.loop(0, h + 2 * PAD)
        def _(y):
            here = pl.ds(pl.multiple_of(y * coarse_pitch, 8), coarse_pitch)
            for ref in (coarse.at[g, 1], coarse_load.at[g], coarse_coef.at[g]):
                ref[here, :] = jnp.zeros((coarse_pitch, LANES), jnp.float32)

    def greet():
        barrier = pltpu.get_barrier_semaphore()
        count = jnp.int32(0)
        for side in range(8):
            count = count + has[side].astype(jnp.int32)

            @pl.when(has[side])
            def _():
                pl.semaphore_signal(barrier, inc=1, device_id=neighbour(side), device_id_type=MESH)

        return barrier, count

    def fine_place(g, b, side, arrives):
        if side >= 2:
            return (column_in if arrives else column_out).at[g, min(b, 1), side - 2]
        if b == 2:
            if arrives:
                return row_in.at[g, side]
            return final.at[g, pl.ds(at(0) if side == 0 else at(height - 1), width), :]
        inner, outer = (0, -1) if side == 0 else (height - 1, height)
        return fine.at[g, b, pl.ds(at(outer if arrives else inner), width), :]

    def fine_copy(g, b, side):
        return pltpu.make_async_remote_copy(
            src_ref=fine_place(g, b, side, False), dst_ref=fine_place(g, b, OPPOSITE[side], True),
            send_sem=fine_send.at[g, min(b, 1), side], recv_sem=fine_recv.at[g, min(b, 1), OPPOSITE[side]],
            device_id=neighbour(side), device_id_type=MESH,
        )

    def fine_arrival(g, b, side):
        place = fine_place(g, b, side, True)
        return pltpu.make_async_remote_copy(
            src_ref=place, dst_ref=place,
            send_sem=fine_send.at[g, min(b, 1), OPPOSITE[side]], recv_sem=fine_recv.at[g, min(b, 1), side],
            device_id=neighbour(side), device_id_type=MESH,
        )

    def values_of(g, b):
        return final.at[g] if b == 2 else fine.at[g, b]

    def send_rows(g, b):
        for side in (0, 1):
            pl.when(has[side])(lambda side=side: fine_copy(g, b, side).start())

    def send_columns(g, b):
        ref = values_of(g, b)
        for side, x in ((2, 0), (3, width - 1)):
            out = column_out.at[g, min(b, 1), side - 2]
            for i in range(height // 8):
                out[pl.ds(8 * i, 8), :] = ref[pl.ds(at(8 * i) + x, 8, stride=pitch), :]
        for side in (2, 3):
            pl.when(has[side])(lambda side=side: fine_copy(g, b, side).start())

    def sent_fine(g, b):
        for side in range(4):
            pl.when(has[side])(lambda side=side: fine_copy(g, b, side).wait_send())

    def receive_fine(g, b):
        ref = values_of(g, b)
        for side in (2, 3, 0, 1):
            pl.when(has[side])(lambda side=side: fine_arrival(g, b, side).wait_recv())
        for side, x in ((2, -1), (3, width)):

            @pl.when(has[side])
            def _():
                column = column_in.at[g, min(b, 1), side - 2]
                for i in range(height // 8):
                    ref[pl.ds(at(8 * i) + x, 8, stride=pitch), :] = column[pl.ds(8 * i, 8), :]

    rows = 8
    chunks = height // rows

    def fine_chunk(g, b, i, finish):
        ref = fine.at[g, b]
        top = i * rows
        for p in range(width // part):
            centre = [
                ref[pl.ds(pl.multiple_of(at(top + r - 1) + p * part, 8), part), :]
                for r in range(rows + 2)
            ]
            for r in range(rows):
                here = at(top + r) + p * part
                around = (centre[r] + centre[r + 2]) + (
                    ref[pl.ds(here - 1, part), :] + ref[pl.ds(here + 1, part), :]
                )
                flat = pl.multiple_of((top + r) * width + p * part, 8)
                finish(top, r, p, pl.multiple_of(here, 8), flat, centre[r + 1], around)

    def fine_loop(g, b, finish, between):
        @pl.loop(0, 2)
        def _(i):
            fine_chunk(g, b, i * (chunks - 1), finish)

        between()

        @pl.loop(1, chunks - 1)
        def _(i):
            fine_chunk(g, b, i, finish)

    def sweep_fine(g, b, new):
        out = values_of(g, new)

        def finish(top, r, p, here, flat, centre, around):
            total = load[g, pl.ds(flat, part), :] + around
            out[pl.ds(here, part), :] = KEEP * centre + coef[g, pl.ds(flat, part), :] * total

        fine_loop(g, b, finish, lambda: send_rows(g, new))
        send_columns(g, new)

    def defect(g, flat, centre, around):
        return (load[g, pl.ds(flat, part), :] + around) - (4.0 + mass[g, pl.ds(flat, part), :]) * centre

    def halve(ref, slot, pair):
        scratch = ref.at[slot]
        scratch[...] = pair
        return scratch[pl.ds(0, part // 2, stride=2), :] + scratch[pl.ds(1, part // 2, stride=2), :]

    def coarsen_mass(g):
        step = 4

        @pl.loop(0, height // step)
        def _(i):
            for p in range(width // part):
                for r in range(0, step, 2):
                    pair = []
                    for s in range(2):
                        flat = pl.multiple_of((i * step + r + s) * width + p * part, 8)
                        here = mass[g, pl.ds(flat, part), :]
                        coef[g, pl.ds(flat, part), :] = WEIGHT / (4.0 + here)
                        pair.append(here)
                    summed = 0.5 * halve(temp, p * (step // 2) + r // 2, pair[0] + pair[1])
                    place = coarse_at(i * (step // 2) + r // 2) + p * (part // 2)
                    coarse_coef[g, pl.ds(pl.multiple_of(place, 8), part // 2), :] = WEIGHT / (4.0 + summed)

    def coarsen_defect(g, b):
        held = {}

        def finish(top, r, p, here, flat, centre, around):
            value = defect(g, flat, centre, around)
            if r % 2 == 0:
                held[p] = value
            else:
                summed = 0.5 * halve(temp, p * 4 + r // 2, held[p] + value)
                place = coarse_at(top // 2 + r // 2) + p * (part // 2)
                coarse_load[g, pl.ds(pl.multiple_of(place, 8), part // 2), :] = summed

        fine_loop(g, b, finish, lambda: send_coarse(g, 1, DEPTHS[0], coarse_load.at[g], (0, 1)))
        send_coarse(g, 1, DEPTHS[0], coarse_load.at[g], (2, 3, 4, 5, 6, 7))

    def blocks(side, depth):
        corner = depth - 1
        dy, dx = OFFSETS[side]
        if dx == 0:
            return (depth, w, 0 if dy < 0 else h - depth, 0, -depth if dy < 0 else h, 0)
        if dy == 0:
            return (h, depth, 0, 0 if dx < 0 else w - depth, 0, -depth if dx < 0 else w)
        return (
            corner, corner, 0 if dy < 0 else h - corner, 0 if dx < 0 else w - corner,
            -corner if dy < 0 else h, -corner if dx < 0 else w,
        )

    def buffers(g, e, side, depth):
        rows, columns = blocks(side, depth)[:2]
        if side < 4:
            return (
                edge_out.at[g, e, side, pl.ds(0, rows * columns), :],
                edge_in.at[g, e, side, pl.ds(0, rows * columns), :],
                edge_in.at[g, e, OPPOSITE[side], pl.ds(0, rows * columns), :],
            )
        return (
            corner_out.at[g, e, side - 4, pl.ds(0, rows * columns), :],
            corner_in.at[g, e, side - 4, pl.ds(0, rows * columns), :],
            corner_in.at[g, e, OPPOSITE[side] - 4, pl.ds(0, rows * columns), :],
        )

    def move(rows, columns, source, source_at, target, target_at):
        step = 8
        if rows % step == 0:

            @pl.loop(0, rows // step)
            def _(i):
                for r in range(step):
                    y = i * step + r
                    target[pl.ds(target_at(y), columns), :] = source[pl.ds(source_at(y), columns), :]
        else:
            for y in range(rows):
                target[pl.ds(target_at(y), columns), :] = source[pl.ds(source_at(y), columns), :]

    def slot(e):
        return 0 if e == 0 else 1 + (e - 1) % 2

    def sides_of(depth):
        return range(8 if depth > 1 else 4)

    def coarse_copy(g, e, side, depth):
        out, _, there = buffers(g, e, side, depth)
        return pltpu.make_async_remote_copy(
            src_ref=out, dst_ref=there,
            send_sem=coarse_send.at[g, slot(e), side], recv_sem=coarse_recv.at[g, slot(e), OPPOSITE[side]],
            device_id=neighbour(side), device_id_type=MESH,
        )

    def coarse_arrival(g, e, side, depth):
        _, here, _ = buffers(g, e, side, depth)
        return pltpu.make_async_remote_copy(
            src_ref=here, dst_ref=here,
            send_sem=coarse_send.at[g, slot(e), OPPOSITE[side]], recv_sem=coarse_recv.at[g, slot(e), side],
            device_id=neighbour(side), device_id_type=MESH,
        )

    def send_coarse(g, e, depth, ref, sides=(4, 5, 6, 7, 0, 1, 2, 3)):
        sides = [side for side in sides if side in sides_of(depth)]
        for side in sides:
            rows, columns, y0, x0, _, _ = blocks(side, depth)
            out = edge_out.at[g, e, side] if side < 4 else corner_out.at[g, e, side - 4]
            move(rows, columns, ref, lambda y: coarse_at(y0 + y) + x0, out, lambda y: y * columns)
        for side in sides:
            pl.when(has[side])(lambda side=side: coarse_copy(g, e, side, depth).start())

    def receive_coarse(g, e, depth, ref):
        for side in sides_of(depth):

            @pl.when(has[side])
            def _():
                coarse_arrival(g, e, side, depth).wait_recv()
                rows, columns, _, _, y1, x1 = blocks(side, depth)
                held = edge_in.at[g, e, side] if side < 4 else corner_in.at[g, e, side - 4]
                move(rows, columns, held, lambda y: y * columns, ref, lambda y: coarse_at(y1 + y) + x1)

    def sent_coarse(g, e, depth):
        for side in sides_of(depth):
            pl.when(has[side])(lambda side=side: coarse_copy(g, e, side, depth).wait_send())

    def first_coarse(g):
        out = coarse.at[g, 0]

        @pl.loop(0, h + 2 * PAD)
        def _(y):
            here = pl.ds(pl.multiple_of(y * coarse_pitch, 8), coarse_pitch)
            out[here, :] = coarse_coef[g, here, :] * coarse_load[g, here, :]

    def sweep_coarse(g, b, valid):
        ref, out = coarse.at[g, b], coarse.at[g, 1 - b]
        rim = (valid + 1) // 2 * 2
        span, left = (w + 8, -4) if valid else (w, 0)
        rows = 4

        @pl.loop(0, (h + 2 * rim) // rows)
        def _(i):
            top = i * rows - rim
            centre = [ref[pl.ds(coarse_at(top + r - 1) + left, span), :] for r in range(rows + 2)]
            for r in range(rows):
                here = coarse_at(top + r) + left
                around = (centre[r] + centre[r + 2]) + (
                    ref[pl.ds(here - 1, span), :] + ref[pl.ds(here + 1, span), :]
                )
                total = coarse_load[g, pl.ds(here, span), :] + around
                out[pl.ds(here, span), :] = KEEP * centre[r + 1] + coarse_coef[g, pl.ds(here, span), :] * total

    def correct(g, b, c):
        ref, values = fine.at[g, b], coarse.at[g, c]

        def spread(slot, value):
            scratch = temp.at[slot]
            scratch[pl.ds(0, part // 2, stride=2), :] = value
            scratch[pl.ds(1, part // 2, stride=2), :] = value
            return scratch[...]

        def add(y, wide, p):
            here = pl.ds(pl.multiple_of(at(y) + p * part, 8), part)
            ref[here, :] = ref[here, :] + wide

        rows = 4

        @pl.loop(0, h // rows)
        def _(i):
            for r in range(rows):
                for p in range(width // part):
                    place = coarse_at(i * rows + r) + p * (part // 2)
                    wide = spread(r * 2 + p, values[pl.ds(pl.multiple_of(place, 8), part // 2), :])
                    for s in range(2):
                        add((i * rows + r) * 2 + s, wide, p)

        for side, y in ((0, -1), (1, height)):
            for p in range(width // part):
                place = coarse_at(-1 if y < 0 else h) + p * (part // 2)
                add(y, spread(side * 2 + p, values[pl.ds(place, part // 2), :]), p)
        for side, x in ((2, -1), (3, width)):
            for p in range(height // part):
                place = coarse_at(p * (part // 2)) + (-1 if x < 0 else w)
                wide = spread(side * 2 + p, values[pl.ds(place, part // 2, stride=coarse_pitch), :])
                for i in range(part // 8):
                    here = pl.ds(at(p * part + 8 * i) + x, 8, stride=pitch)
                    ref[here, :] = ref[here, :] + wide[8 * i : 8 * i + 8]

    both = range(GROUPS)
    barrier, count = greet()
    for g in both:
        start_values(g)
    for g in both:
        start_terms(g)
    clear_rows()
    pl.semaphore_wait(barrier, count)
    for g in both:
        wait_input(0, g)
        send_rows(g, 0)
        send_columns(g, 0)
    for g in both:
        clear_rest(g)
        wait_input(1, g)
        coarsen_mass(g)
        send_coarse(g, 0, DEPTHS[0], coarse_coef.at[g], PARTS[0])
        wait_input(2, g)
    now = 0
    for sweep in range(BEFORE):
        for g in both:
            receive_fine(g, now)
            if sweep >= 1:
                sent_fine(g, 1 - now)
            sweep_fine(g, now, 1 - now)
            send_coarse(g, 0, DEPTHS[0], coarse_coef.at[g], PARTS[1 + sweep])
        now = 1 - now
    for g in both:
        receive_fine(g, now)
        coarsen_defect(g, now)
    for g in both:
        receive_coarse(g, 0, DEPTHS[0], coarse_coef.at[g])
    inner, c = 1, 0
    for e, depth in enumerate(DEPTHS):
        last = e == len(DEPTHS) - 1
        count = depth - 1 if last else depth
        for g in both:
            b = c
            if e == 0:
                receive_coarse(g, 1, depth, coarse_load.at[g])
                first_coarse(g)
            else:
                receive_coarse(g, 1 + e, depth, coarse.at[g, b])
            for i in range(count):
                sweep_coarse(g, b, depth - 1 - i)
                b = 1 - b
            if not last:
                if e >= 1:
                    sent_coarse(g, e, DEPTHS[e - 1])
                send_coarse(g, 2 + e, DEPTHS[e + 1], coarse.at[g, b])
            else:
                sent_fine(g, now)
                correct(g, now, b)
                sent_fine(g, 1 - now)
                sweep_fine(g, now, 1 - now)
        c = (c + count) % 2
        inner += count
    assert inner == INNER and now == 1
    for g in both:
        receive_fine(g, 0)
        sweep_fine(g, 0, 2)
        for e in (0, len(DEPTHS) - 1, len(DEPTHS)):
            sent_coarse(g, e, DEPTHS[max(e - 1, 0)])
    for g in both:
        receive_fine(g, 2)
        for side, y in ((0, -1), (1, height)):

            @pl.when(has[side])
            def _():
                final[g, pl.ds(at(y), width), :] = row_in[g, side]

        sent_fine(g, 0)
        sent_fine(g, 2)


def finish_kernel(height, width, final, blocked, load, mass, sol_hbm, rem_hbm, rem, sol_sem, rem_sem):
    pitch, part, rows = width + 8, min(32, width), 8
    chunks = 2 if height % (2 * rows) == 0 else 1
    span = height // chunks

    def group_lanes(g):
        return pl.ds(g * LANES, LANES)

    def at(y):
        return (y + 1) * pitch + 8

    def remaining_copy(g, c):
        here = pl.ds(c * span * width, span * width)
        return pltpu.make_async_copy(rem.at[g, here, :], rem_hbm.at[here, group_lanes(g)], rem_sem.at[g, c])

    def solution_copy(g):
        own = blocked.at[g, pl.ds(1, height), pl.ds(8, width), :]
        return pltpu.make_async_copy(own, sol_hbm.at[:, :, group_lanes(g)], sol_sem.at[g])

    for g in range(GROUPS):
        solution_copy(g).start()
    for g in range(GROUPS):
        for c in range(chunks):

            @pl.loop(0, span // rows)
            def _(i):
                top = c * span + i * rows
                for p in range(width // part):
                    centre = [
                        final[g, pl.ds(pl.multiple_of(at(top + r - 1) + p * part, 8), part), :]
                        for r in range(rows + 2)
                    ]
                    for r in range(rows):
                        here = at(top + r) + p * part
                        around = (centre[r] + centre[r + 2]) + (
                            final[g, pl.ds(here - 1, part), :] + final[g, pl.ds(here + 1, part), :]
                        )
                        flat = pl.ds(pl.multiple_of((top + r) * width + p * part, 8), part)
                        rem[g, flat, :] = (load[g, flat, :] + around) - (4.0 + mass[g, flat, :]) * centre[r + 1]

            remaining_copy(g, c).start()
    for g in range(GROUPS):
        for c in range(chunks):
            remaining_copy(g, c).wait()
        solution_copy(g).wait()


def body(load_terms, start_values, reaction_rate):
    height, width, layers = load_terms.shape
    h, w = height // 2, width // 2
    flat = (height * width, layers)
    fine_rows = (height + 3) * (width + 8)
    coarse_rows = (h + 2 * PAD) * (w + 16)
    exchanges = len(DEPTHS) + 1
    edge = max(DEPTHS) * max(h, w)
    corner = -(-((max(DEPTHS) - 1) ** 2) // 8) * 8
    f32 = jnp.float32
    any_space = pl.BlockSpec(memory_space=pl.ANY)
    vmem_space = pl.BlockSpec(memory_space=pltpu.VMEM)
    cells = height * width
    held = pl.pallas_call(
        functools.partial(kernel, height, width),
        out_shape=[
            pltpu.VMEM((GROUPS, fine_rows, LANES), f32),
            pltpu.VMEM((GROUPS, cells, LANES), f32),
            pltpu.VMEM((GROUPS, cells, LANES), f32),
        ],
        in_specs=[any_space] * 3,
        out_specs=[vmem_space] * 3,
        scratch_shapes=[
            pltpu.VMEM((GROUPS, 2, fine_rows, LANES), f32),
            pltpu.VMEM((GROUPS, cells, LANES), f32),
            pltpu.VMEM((GROUPS, 2, width, LANES), f32),
            pltpu.VMEM((GROUPS, 2, 2, height, LANES), f32),
            pltpu.VMEM((GROUPS, 2, 2, height, LANES), f32),
            pltpu.VMEM((GROUPS, 2, coarse_rows, LANES), f32),
            pltpu.VMEM((GROUPS, coarse_rows, LANES), f32),
            pltpu.VMEM((GROUPS, coarse_rows, LANES), f32),
            pltpu.VMEM((GROUPS, exchanges, 4, edge, LANES), f32),
            pltpu.VMEM((GROUPS, exchanges, 4, edge, LANES), f32),
            pltpu.VMEM((GROUPS, exchanges, 4, corner, LANES), f32),
            pltpu.VMEM((GROUPS, exchanges, 4, corner, LANES), f32),
            pltpu.VMEM((8, min(32, width), LANES), f32),
            pltpu.SemaphoreType.DMA((3, GROUPS)),
            pltpu.SemaphoreType.DMA((GROUPS, 2, 4)),
            pltpu.SemaphoreType.DMA((GROUPS, 2, 4)),
            pltpu.SemaphoreType.DMA((GROUPS, 3, 8)),
            pltpu.SemaphoreType.DMA((GROUPS, 3, 8)),
        ],
        compiler_params=pltpu.CompilerParams(
            collective_id=0, has_side_effects=True, vmem_limit_bytes=48 * 1024 * 1024
        ),
    )(load_terms.reshape(flat), start_values.reshape(flat), reaction_rate.reshape(flat))
    results = pl.pallas_call(
        functools.partial(finish_kernel, height, width),
        out_shape=[
            jax.ShapeDtypeStruct((height, width, layers), f32),
            jax.ShapeDtypeStruct(flat, f32),
        ],
        in_specs=[vmem_space] * 4,
        out_specs=[any_space] * 2,
        scratch_shapes=[
            pltpu.VMEM((GROUPS, cells, LANES), f32),
            pltpu.SemaphoreType.DMA((GROUPS,)),
            pltpu.SemaphoreType.DMA((GROUPS, 2)),
        ],
        compiler_params=pltpu.CompilerParams(vmem_limit_bytes=24 * 1024 * 1024),
    )(held[0], held[0].reshape(GROUPS, height + 3, width + 8, LANES), held[1], held[2])
    return tuple(result.reshape(height, width, layers) for result in results)


def solution(mesh):
    spec = P("band", "lane", None)
    return jax.shard_map(
        body, mesh=mesh, in_specs=(spec, spec, spec), out_specs=(spec, spec), check_vma=False
    )
```

```python
import functools

import jax
import jax.numpy as jnp
import numpy as np
from jax import lax
from jax.experimental import pallas as pl
from jax.experimental.pallas import tpu as pltpu
from jax.sharding import PartitionSpec as P

BEFORE = 3
INNER = 13
LANES = 128
GROUPS = 2
DEPTHS = (2, 3, 2, 3, 3)
PARTS = ((), (0, 1), (2, 4, 5), (3, 6, 7))
PAD = 5
WEIGHT = np.float32(0.8)
KEEP = np.float32(1.0) - WEIGHT
MESH = pl.DeviceIdType.MESH

OFFSETS = ((-1, 0), (1, 0), (0, -1), (0, 1), (-1, -1), (-1, 1), (1, -1), (1, 1))
OPPOSITE = (1, 0, 3, 2, 7, 6, 5, 4)


def kernel(
    height, width, load_hbm, start_hbm, mass_hbm, final, load, mass,
    fine, coef, row_in, column_out, column_in, coarse, coarse_load, coarse_coef,
    edge_out, edge_in, corner_out, corner_in, temp,
    load_sem, fine_send, fine_recv, coarse_send, coarse_recv,
):
    h, w = height // 2, width // 2
    pitch, coarse_pitch = width + 8, w + 16
    cells = height * width
    part = min(32, width)
    band, lane = lax.axis_index("band"), lax.axis_index("lane")
    bands, lanes = lax.axis_size("band"), lax.axis_size("lane")
    inside = {-1: (band > 0, lane > 0), 1: (band < bands - 1, lane < lanes - 1)}
    has = []
    for dy, dx in OFFSETS:
        if dx == 0:
            has.append(inside[dy][0])
        elif dy == 0:
            has.append(inside[dx][1])
        else:
            has.append(jnp.logical_and(inside[dy][0], inside[dx][1]))

    def neighbour(side):
        dy, dx = OFFSETS[side]
        return (band + dy, lane + dx)

    def at(y):
        return (y + 1) * pitch + 8

    def coarse_at(y):
        return (y + PAD) * coarse_pitch + 8

    def group_lanes(g):
        return pl.ds(g * LANES, LANES)

    def start_values(g):
        target = fine.at[g, 0]

        @pl.loop(0, height)
        def _(y):
            pltpu.make_async_copy(
                start_hbm.at[pl.ds(pl.multiple_of(y * width, 8), width), group_lanes(g)],
                target.at[pl.ds(pl.multiple_of(at(y), 8), width), :],
                load_sem.at[0, g],
            ).start()

    def start_terms(g):
        pltpu.make_async_copy(mass_hbm.at[:, group_lanes(g)], mass.at[g], load_sem.at[1, g]).start()
        pltpu.make_async_copy(load_hbm.at[:, group_lanes(g)], load.at[g], load_sem.at[2, g]).start()

    def wait_input(which, g):
        source, target = ((start_hbm, coef), (mass_hbm, mass), (load_hbm, load))[which]
        pltpu.make_async_copy(source.at[:, group_lanes(g)], target.at[g], load_sem.at[which, g]).wait()

    def clear_rows():
        for side, y in ((0, -1), (1, height)):

            @pl.when(jnp.logical_not(has[side]))
            def _():
                for g in range(GROUPS):
                    for b in range(2):
                        fine[g, b, pl.ds(at(y), width), :] = jnp.zeros((width, LANES), jnp.float32)

    def clear_rest(g):
        zero8 = jnp.zeros((8, LANES), jnp.float32)
        step = 8

        @pl.loop(0, height // step)
        def _(i):
            for r in range(step):
                here = pl.ds(pl.multiple_of((i * step + r + 1) * pitch, 8), 8)
                fine[g, 0, here, :] = zero8
                fine[g, 1, here, :] = zero8
                final[g, here, :] = zero8

        for ref in (fine.at[g, 0], fine.at[g, 1], final.at[g]):
            for y in (0, height + 1, height + 2):
                ref[pl.ds(y * pitch, 8), :] = zero8
        for y in (-1, height):
            final[g, pl.ds(at(y), width), :] = jnp.zeros((width, LANES), jnp.float32)

        @pl.loop(0, h + 2 * PAD)
        def _(y):
            here = pl.ds(pl.multiple_of(y * coarse_pitch, 8), coarse_pitch)
            for ref in (coarse.at[g, 1], coarse_load.at[g], coarse_coef.at[g]):
                ref[here, :] = jnp.zeros((coarse_pitch, LANES), jnp.float32)

    def greet():
        barrier = pltpu.get_barrier_semaphore()
        count = jnp.int32(0)
        for side in range(8):
            count = count + has[side].astype(jnp.int32)

            @pl.when(has[side])
            def _():
                pl.semaphore_signal(barrier, inc=1, device_id=neighbour(side), device_id_type=MESH)

        return barrier, count

    def fine_place(g, b, side, arrives):
        if side >= 2:
            return (column_in if arrives else column_out).at[g, min(b, 1), side - 2]
        if b == 2:
            if arrives:
                return row_in.at[g, side]
            return final.at[g, pl.ds(at(0) if side == 0 else at(height - 1), width), :]
        inner, outer = (0, -1) if side == 0 else (height - 1, height)
        return fine.at[g, b, pl.ds(at(outer if arrives else inner), width), :]

    def fine_copy(g, b, side):
        return pltpu.make_async_remote_copy(
            src_ref=fine_place(g, b, side, False), dst_ref=fine_place(g, b, OPPOSITE[side], True),
            send_sem=fine_send.at[g, min(b, 1), side], recv_sem=fine_recv.at[g, min(b, 1), OPPOSITE[side]],
            device_id=neighbour(side), device_id_type=MESH,
        )

    def fine_arrival(g, b, side):
        place = fine_place(g, b, side, True)
        return pltpu.make_async_remote_copy(
            src_ref=place, dst_ref=place,
            send_sem=fine_send.at[g, min(b, 1), OPPOSITE[side]], recv_sem=fine_recv.at[g, min(b, 1), side],
            device_id=neighbour(side), device_id_type=MESH,
        )

    def values_of(g, b):
        return final.at[g] if b == 2 else fine.at[g, b]

    def send_rows(g, b):
        for side in (0, 1):
            pl.when(has[side])(lambda side=side: fine_copy(g, b, side).start())

    def send_columns(g, b):
        ref = values_of(g, b)
        for side, x in ((2, 0), (3, width - 1)):
            out = column_out.at[g, min(b, 1), side - 2]
            for i in range(height // 8):
                out[pl.ds(8 * i, 8), :] = ref[pl.ds(at(8 * i) + x, 8, stride=pitch), :]
        for side in (2, 3):
            pl.when(has[side])(lambda side=side: fine_copy(g, b, side).start())

    def sent_fine(g, b):
        for side in range(4):
            pl.when(has[side])(lambda side=side: fine_copy(g, b, side).wait_send())

    def receive_fine(g, b):
        ref = values_of(g, b)
        for side in (2, 3, 0, 1):
            pl.when(has[side])(lambda side=side: fine_arrival(g, b, side).wait_recv())
        for side, x in ((2, -1), (3, width)):

            @pl.when(has[side])
            def _():
                column = column_in.at[g, min(b, 1), side - 2]
                for i in range(height // 8):
                    ref[pl.ds(at(8 * i) + x, 8, stride=pitch), :] = column[pl.ds(8 * i, 8), :]

    rows = 8
    chunks = height // rows

    def fine_chunk(g, b, i, finish):
        ref = fine.at[g, b]
        top = i * rows
        for p in range(width // part):
            centre = [
                ref[pl.ds(pl.multiple_of(at(top + r - 1) + p * part, 8), part), :]
                for r in range(rows + 2)
            ]
            for r in range(rows):
                here = at(top + r) + p * part
                around = (centre[r] + centre[r + 2]) + (
                    ref[pl.ds(here - 1, part), :] + ref[pl.ds(here + 1, part), :]
                )
                flat = pl.multiple_of((top + r) * width + p * part, 8)
                finish(top, r, p, pl.multiple_of(here, 8), flat, centre[r + 1], around)

    def fine_loop(g, b, finish, between):
        @pl.loop(0, 2)
        def _(i):
            fine_chunk(g, b, i * (chunks - 1), finish)

        between()

        @pl.loop(1, chunks - 1)
        def _(i):
            fine_chunk(g, b, i, finish)

    def sweep_fine(g, b, new):
        out = values_of(g, new)

        def finish(top, r, p, here, flat, centre, around):
            total = load[g, pl.ds(flat, part), :] + around
            out[pl.ds(here, part), :] = KEEP * centre + coef[g, pl.ds(flat, part), :] * total

        fine_loop(g, b, finish, lambda: send_rows(g, new))
        send_columns(g, new)

    def defect(g, flat, centre, around):
        return (load[g, pl.ds(flat, part), :] + around) - (4.0 + mass[g, pl.ds(flat, part), :]) * centre

    def halve(ref, slot, pair):
        scratch = ref.at[slot]
        scratch[...] = pair
        return scratch[pl.ds(0, part // 2, stride=2), :] + scratch[pl.ds(1, part // 2, stride=2), :]

    def coarsen_mass(g):
        step = 4

        @pl.loop(0, height // step)
        def _(i):
            for p in range(width // part):
                for r in range(0, step, 2):
                    pair = []
                    for s in range(2):
                        flat = pl.multiple_of((i * step + r + s) * width + p * part, 8)
                        here = mass[g, pl.ds(flat, part), :]
                        coef[g, pl.ds(flat, part), :] = WEIGHT / (4.0 + here)
                        pair.append(here)
                    summed = 0.5 * halve(temp, p * (step // 2) + r // 2, pair[0] + pair[1])
                    place = coarse_at(i * (step // 2) + r // 2) + p * (part // 2)
                    coarse_coef[g, pl.ds(pl.multiple_of(place, 8), part // 2), :] = WEIGHT / (4.0 + summed)

    def coarsen_defect(g, b):
        held = {}

        def finish(top, r, p, here, flat, centre, around):
            value = defect(g, flat, centre, around)
            if r % 2 == 0:
                held[p] = value
            else:
                summed = 0.5 * halve(temp, p * 4 + r // 2, held[p] + value)
                place = coarse_at(top // 2 + r // 2) + p * (part // 2)
                coarse_load[g, pl.ds(pl.multiple_of(place, 8), part // 2), :] = summed

        fine_loop(g, b, finish, lambda: send_coarse(g, 1, DEPTHS[0], coarse_load.at[g], (4, 5, 6, 7, 0, 1)))
        send_coarse(g, 1, DEPTHS[0], coarse_load.at[g], (2, 3))

    def blocks(side, depth):
        corner = depth - 1
        dy, dx = OFFSETS[side]
        if dx == 0:
            return (depth, w, 0 if dy < 0 else h - depth, 0, -depth if dy < 0 else h, 0)
        if dy == 0:
            return (h, depth, 0, 0 if dx < 0 else w - depth, 0, -depth if dx < 0 else w)
        return (
            corner, corner, 0 if dy < 0 else h - corner, 0 if dx < 0 else w - corner,
            -corner if dy < 0 else h, -corner if dx < 0 else w,
        )

    def buffers(g, e, side, depth):
        rows, columns = blocks(side, depth)[:2]
        if side < 4:
            return (
                edge_out.at[g, e, side, pl.ds(0, rows * columns), :],
                edge_in.at[g, e, side, pl.ds(0, rows * columns), :],
                edge_in.at[g, e, OPPOSITE[side], pl.ds(0, rows * columns), :],
            )
        return (
            corner_out.at[g, e, side - 4, pl.ds(0, rows * columns), :],
            corner_in.at[g, e, side - 4, pl.ds(0, rows * columns), :],
            corner_in.at[g, e, OPPOSITE[side] - 4, pl.ds(0, rows * columns), :],
        )

    def move(rows, columns, source, source_at, target, target_at):
        step = 8
        if rows % step == 0:

            @pl.loop(0, rows // step)
            def _(i):
                for r in range(step):
                    y = i * step + r
                    target[pl.ds(target_at(y), columns), :] = source[pl.ds(source_at(y), columns), :]
        else:
            for y in range(rows):
                target[pl.ds(target_at(y), columns), :] = source[pl.ds(source_at(y), columns), :]

    def slot(e):
        return 0 if e == 0 else 1 + (e - 1) % 2

    def sides_of(depth):
        return range(8 if depth > 1 else 4)

    def coarse_copy(g, e, side, depth):
        out, _, there = buffers(g, e, side, depth)
        return pltpu.make_async_remote_copy(
            src_ref=out, dst_ref=there,
            send_sem=coarse_send.at[g, slot(e), side], recv_sem=coarse_recv.at[g, slot(e), OPPOSITE[side]],
            device_id=neighbour(side), device_id_type=MESH,
        )

    def coarse_arrival(g, e, side, depth):
        _, here, _ = buffers(g, e, side, depth)
        return pltpu.make_async_remote_copy(
            src_ref=here, dst_ref=here,
            send_sem=coarse_send.at[g, slot(e), OPPOSITE[side]], recv_sem=coarse_recv.at[g, slot(e), side],
            device_id=neighbour(side), device_id_type=MESH,
        )

    def send_coarse(g, e, depth, ref, sides=(4, 5, 6, 7, 0, 1, 2, 3)):
        sides = [side for side in sides if side in sides_of(depth)]
        for side in sides:
            rows, columns, y0, x0, _, _ = blocks(side, depth)
            out = edge_out.at[g, e, side] if side < 4 else corner_out.at[g, e, side - 4]
            move(rows, columns, ref, lambda y: coarse_at(y0 + y) + x0, out, lambda y: y * columns)
        for side in sides:
            pl.when(has[side])(lambda side=side: coarse_copy(g, e, side, depth).start())

    def receive_coarse(g, e, depth, ref):
        for side in (2, 3, *range(4, len(sides_of(depth))), 0, 1):

            @pl.when(has[side])
            def _():
                coarse_arrival(g, e, side, depth).wait_recv()
                rows, columns, _, _, y1, x1 = blocks(side, depth)
                held = edge_in.at[g, e, side] if side < 4 else corner_in.at[g, e, side - 4]
                move(rows, columns, held, lambda y: y * columns, ref, lambda y: coarse_at(y1 + y) + x1)

    def sent_coarse(g, e, depth):
        for side in sides_of(depth):
            pl.when(has[side])(lambda side=side: coarse_copy(g, e, side, depth).wait_send())

    def first_coarse(g):
        out = coarse.at[g, 0]

        @pl.loop(0, h + 2 * PAD)
        def _(y):
            here = pl.ds(pl.multiple_of(y * coarse_pitch, 8), coarse_pitch)
            out[here, :] = coarse_coef[g, here, :] * coarse_load[g, here, :]

    def sweep_coarse(g, b, valid):
        ref, out = coarse.at[g, b], coarse.at[g, 1 - b]
        rim = (valid + 1) // 2 * 2
        span, left = (w + 8, -4) if valid else (w, 0)
        rows = 4

        @pl.loop(0, (h + 2 * rim) // rows)
        def _(i):
            top = i * rows - rim
            centre = [ref[pl.ds(coarse_at(top + r - 1) + left, span), :] for r in range(rows + 2)]
            for r in range(rows):
                here = coarse_at(top + r) + left
                around = (centre[r] + centre[r + 2]) + (
                    ref[pl.ds(here - 1, span), :] + ref[pl.ds(here + 1, span), :]
                )
                total = coarse_load[g, pl.ds(here, span), :] + around
                out[pl.ds(here, span), :] = KEEP * centre[r + 1] + coarse_coef[g, pl.ds(here, span), :] * total

    def correct(g, b, c):
        ref, values = fine.at[g, b], coarse.at[g, c]

        def spread(slot, value):
            scratch = temp.at[slot]
            scratch[pl.ds(0, part // 2, stride=2), :] = value
            scratch[pl.ds(1, part // 2, stride=2), :] = value
            return scratch[...]

        def add(y, wide, p):
            here = pl.ds(pl.multiple_of(at(y) + p * part, 8), part)
            ref[here, :] = ref[here, :] + wide

        rows = 4

        @pl.loop(0, h // rows)
        def _(i):
            for r in range(rows):
                for p in range(width // part):
                    place = coarse_at(i * rows + r) + p * (part // 2)
                    wide = spread(r * 2 + p, values[pl.ds(pl.multiple_of(place, 8), part // 2), :])
                    for s in range(2):
                        add((i * rows + r) * 2 + s, wide, p)

        for side, y in ((0, -1), (1, height)):
            for p in range(width // part):
                place = coarse_at(-1 if y < 0 else h) + p * (part // 2)
                add(y, spread(side * 2 + p, values[pl.ds(place, part // 2), :]), p)
        for side, x in ((2, -1), (3, width)):
            for p in range(height // part):
                place = coarse_at(p * (part // 2)) + (-1 if x < 0 else w)
                wide = spread(side * 2 + p, values[pl.ds(place, part // 2, stride=coarse_pitch), :])
                for i in range(part // 8):
                    here = pl.ds(at(p * part + 8 * i) + x, 8, stride=pitch)
                    ref[here, :] = ref[here, :] + wide[8 * i : 8 * i + 8]

    both = range(GROUPS)
    barrier, count = greet()
    for g in both:
        start_values(g)
    for g in both:
        start_terms(g)
    clear_rows()
    pl.semaphore_wait(barrier, count)
    for g in both:
        wait_input(0, g)
        send_rows(g, 0)
        send_columns(g, 0)
    for g in both:
        clear_rest(g)
        wait_input(1, g)
        coarsen_mass(g)
        send_coarse(g, 0, DEPTHS[0], coarse_coef.at[g], PARTS[0])
        wait_input(2, g)
    now = 0
    for sweep in range(BEFORE):
        for g in both:
            receive_fine(g, now)
            if sweep >= 1:
                sent_fine(g, 1 - now)
            sweep_fine(g, now, 1 - now)
            send_coarse(g, 0, DEPTHS[0], coarse_coef.at[g], PARTS[1 + sweep])
        now = 1 - now
    for g in both:
        receive_fine(g, now)
        coarsen_defect(g, now)
    for g in both:
        receive_coarse(g, 0, DEPTHS[0], coarse_coef.at[g])
    inner, c = 1, 0
    for e, depth in enumerate(DEPTHS):
        last = e == len(DEPTHS) - 1
        count = depth - 1 if last else depth
        for g in both:
            b = c
            if e == 0:
                receive_coarse(g, 1, depth, coarse_load.at[g])
                first_coarse(g)
            else:
                receive_coarse(g, 1 + e, depth, coarse.at[g, b])
            for i in range(count):
                sweep_coarse(g, b, depth - 1 - i)
                b = 1 - b
            if not last:
                if e >= 1:
                    sent_coarse(g, e, DEPTHS[e - 1])
                send_coarse(g, 2 + e, DEPTHS[e + 1], coarse.at[g, b])
            else:
                sent_fine(g, now)
                correct(g, now, b)
                sent_fine(g, 1 - now)
                sweep_fine(g, now, 1 - now)
        c = (c + count) % 2
        inner += count
    assert inner == INNER and now == 1
    for g in both:
        receive_fine(g, 0)
        sweep_fine(g, 0, 2)
        for e in (0, len(DEPTHS) - 1, len(DEPTHS)):
            sent_coarse(g, e, DEPTHS[max(e - 1, 0)])
    for g in both:
        receive_fine(g, 2)
        for side, y in ((0, -1), (1, height)):

            @pl.when(has[side])
            def _():
                final[g, pl.ds(at(y), width), :] = row_in[g, side]

        sent_fine(g, 0)
        sent_fine(g, 2)


def finish_kernel(height, width, final, blocked, load, mass, sol_hbm, rem_hbm, rem, sol_sem, rem_sem):
    pitch, part, rows = width + 8, min(32, width), 8
    chunks = 2 if height % (2 * rows) == 0 else 1
    span = height // chunks

    def group_lanes(g):
        return pl.ds(g * LANES, LANES)

    def at(y):
        return (y + 1) * pitch + 8

    def remaining_copy(g, c):
        here = pl.ds(c * span * width, span * width)
        return pltpu.make_async_copy(rem.at[g, here, :], rem_hbm.at[here, group_lanes(g)], rem_sem.at[g, c])

    def solution_copy(g):
        own = blocked.at[g, pl.ds(1, height), pl.ds(8, width), :]
        return pltpu.make_async_copy(own, sol_hbm.at[:, :, group_lanes(g)], sol_sem.at[g])

    for g in range(GROUPS):
        solution_copy(g).start()
    for g in range(GROUPS):
        for c in range(chunks):

            @pl.loop(0, span // rows)
            def _(i):
                top = c * span + i * rows
                for p in range(width // part):
                    centre = [
                        final[g, pl.ds(pl.multiple_of(at(top + r - 1) + p * part, 8), part), :]
                        for r in range(rows + 2)
                    ]
                    for r in range(rows):
                        here = at(top + r) + p * part
                        around = (centre[r] + centre[r + 2]) + (
                            final[g, pl.ds(here - 1, part), :] + final[g, pl.ds(here + 1, part), :]
                        )
                        flat = pl.ds(pl.multiple_of((top + r) * width + p * part, 8), part)
                        rem[g, flat, :] = (load[g, flat, :] + around) - (4.0 + mass[g, flat, :]) * centre[r + 1]

            remaining_copy(g, c).start()
    for g in range(GROUPS):
        for c in range(chunks):
            remaining_copy(g, c).wait()
        solution_copy(g).wait()


def body(load_terms, start_values, reaction_rate):
    height, width, layers = load_terms.shape
    h, w = height // 2, width // 2
    flat = (height * width, layers)
    fine_rows = (height + 3) * (width + 8)
    coarse_rows = (h + 2 * PAD) * (w + 16)
    exchanges = len(DEPTHS) + 1
    edge = max(DEPTHS) * max(h, w)
    corner = -(-((max(DEPTHS) - 1) ** 2) // 8) * 8
    f32 = jnp.float32
    any_space = pl.BlockSpec(memory_space=pl.ANY)
    vmem_space = pl.BlockSpec(memory_space=pltpu.VMEM)
    cells = height * width
    held = pl.pallas_call(
        functools.partial(kernel, height, width),
        out_shape=[
            pltpu.VMEM((GROUPS, fine_rows, LANES), f32),
            pltpu.VMEM((GROUPS, cells, LANES), f32),
            pltpu.VMEM((GROUPS, cells, LANES), f32),
        ],
        in_specs=[any_space] * 3,
        out_specs=[vmem_space] * 3,
        scratch_shapes=[
            pltpu.VMEM((GROUPS, 2, fine_rows, LANES), f32),
            pltpu.VMEM((GROUPS, cells, LANES), f32),
            pltpu.VMEM((GROUPS, 2, width, LANES), f32),
            pltpu.VMEM((GROUPS, 2, 2, height, LANES), f32),
            pltpu.VMEM((GROUPS, 2, 2, height, LANES), f32),
            pltpu.VMEM((GROUPS, 2, coarse_rows, LANES), f32),
            pltpu.VMEM((GROUPS, coarse_rows, LANES), f32),
            pltpu.VMEM((GROUPS, coarse_rows, LANES), f32),
            pltpu.VMEM((GROUPS, exchanges, 4, edge, LANES), f32),
            pltpu.VMEM((GROUPS, exchanges, 4, edge, LANES), f32),
            pltpu.VMEM((GROUPS, exchanges, 4, corner, LANES), f32),
            pltpu.VMEM((GROUPS, exchanges, 4, corner, LANES), f32),
            pltpu.VMEM((8, min(32, width), LANES), f32),
            pltpu.SemaphoreType.DMA((3, GROUPS)),
            pltpu.SemaphoreType.DMA((GROUPS, 2, 4)),
            pltpu.SemaphoreType.DMA((GROUPS, 2, 4)),
            pltpu.SemaphoreType.DMA((GROUPS, 3, 8)),
            pltpu.SemaphoreType.DMA((GROUPS, 3, 8)),
        ],
        compiler_params=pltpu.CompilerParams(
            collective_id=0, has_side_effects=True, vmem_limit_bytes=48 * 1024 * 1024
        ),
    )(load_terms.reshape(flat), start_values.reshape(flat), reaction_rate.reshape(flat))
    results = pl.pallas_call(
        functools.partial(finish_kernel, height, width),
        out_shape=[
            jax.ShapeDtypeStruct((height, width, layers), f32),
            jax.ShapeDtypeStruct(flat, f32),
        ],
        in_specs=[vmem_space] * 4,
        out_specs=[any_space] * 2,
        scratch_shapes=[
            pltpu.VMEM((GROUPS, cells, LANES), f32),
            pltpu.SemaphoreType.DMA((GROUPS,)),
            pltpu.SemaphoreType.DMA((GROUPS, 2)),
        ],
        compiler_params=pltpu.CompilerParams(vmem_limit_bytes=24 * 1024 * 1024),
    )(held[0], held[0].reshape(GROUPS, height + 3, width + 8, LANES), held[1], held[2])
    return tuple(result.reshape(height, width, layers) for result in results)


def solution(mesh):
    spec = P("band", "lane", None)
    return jax.shard_map(
        body, mesh=mesh, in_specs=(spec, spec, spec), out_specs=(spec, spec), check_vma=False
    )
```

```python
import functools

import jax
import jax.numpy as jnp
import numpy as np
from jax import lax
from jax.experimental import pallas as pl
from jax.experimental.pallas import tpu as pltpu
from jax.sharding import PartitionSpec as P

BEFORE = 3
INNER = 13
LANES = 128
GROUPS = 2
DEPTHS = (2, 3, 2, 3, 3)
PARTS = ((), (0, 1), (2, 4, 5), (3, 6, 7))
PAD = 5
WEIGHT = np.float32(0.8)
KEEP = np.float32(1.0) - WEIGHT
MESH = pl.DeviceIdType.MESH

OFFSETS = ((-1, 0), (1, 0), (0, -1), (0, 1), (-1, -1), (-1, 1), (1, -1), (1, 1))
OPPOSITE = (1, 0, 3, 2, 7, 6, 5, 4)


def kernel(
    height, width, load_hbm, start_hbm, mass_hbm, final, load, mass,
    fine, coef, row_in, column_out, column_in, coarse, coarse_load, coarse_coef,
    edge_out, edge_in, corner_out, corner_in, temp,
    load_sem, fine_send, fine_recv, coarse_send, coarse_recv,
):
    h, w = height // 2, width // 2
    pitch, coarse_pitch = width + 8, w + 16
    cells = height * width
    part = min(32, width)
    band, lane = lax.axis_index("band"), lax.axis_index("lane")
    bands, lanes = lax.axis_size("band"), lax.axis_size("lane")
    inside = {-1: (band > 0, lane > 0), 1: (band < bands - 1, lane < lanes - 1)}
    has = []
    for dy, dx in OFFSETS:
        if dx == 0:
            has.append(inside[dy][0])
        elif dy == 0:
            has.append(inside[dx][1])
        else:
            has.append(jnp.logical_and(inside[dy][0], inside[dx][1]))

    def neighbour(side):
        dy, dx = OFFSETS[side]
        return (band + dy, lane + dx)

    def at(y):
        return (y + 1) * pitch + 8

    def coarse_at(y):
        return (y + PAD) * coarse_pitch + 8

    def group_lanes(g):
        return pl.ds(g * LANES, LANES)

    def start_values(g):
        target = fine.at[g, 0]

        @pl.loop(0, height)
        def _(y):
            pltpu.make_async_copy(
                start_hbm.at[pl.ds(pl.multiple_of(y * width, 8), width), group_lanes(g)],
                target.at[pl.ds(pl.multiple_of(at(y), 8), width), :],
                load_sem.at[0, g],
            ).start()

    def start_terms(g):
        pltpu.make_async_copy(mass_hbm.at[:, group_lanes(g)], mass.at[g], load_sem.at[1, g]).start()
        pltpu.make_async_copy(load_hbm.at[:, group_lanes(g)], load.at[g], load_sem.at[2, g]).start()

    def wait_input(which, g):
        source, target = ((start_hbm, coef), (mass_hbm, mass), (load_hbm, load))[which]
        pltpu.make_async_copy(source.at[:, group_lanes(g)], target.at[g], load_sem.at[which, g]).wait()

    def clear_rows():
        for side, y in ((0, -1), (1, height)):

            @pl.when(jnp.logical_not(has[side]))
            def _():
                for g in range(GROUPS):
                    for b in range(2):
                        fine[g, b, pl.ds(at(y), width), :] = jnp.zeros((width, LANES), jnp.float32)

    def clear_rest(g):
        zero8 = jnp.zeros((8, LANES), jnp.float32)
        step = 8

        @pl.loop(0, height // step)
        def _(i):
            for r in range(step):
                here = pl.ds(pl.multiple_of((i * step + r + 1) * pitch, 8), 8)
                fine[g, 0, here, :] = zero8
                fine[g, 1, here, :] = zero8
                final[g, here, :] = zero8

        for ref in (fine.at[g, 0], fine.at[g, 1], final.at[g]):
            for y in (0, height + 1, height + 2):
                ref[pl.ds(y * pitch, 8), :] = zero8
        for y in (-1, height):
            final[g, pl.ds(at(y), width), :] = jnp.zeros((width, LANES), jnp.float32)

        @pl.loop(0, h + 2 * PAD)
        def _(y):
            here = pl.ds(pl.multiple_of(y * coarse_pitch, 8), coarse_pitch)
            for ref in (coarse.at[g, 1], coarse_load.at[g], coarse_coef.at[g]):
                ref[here, :] = jnp.zeros((coarse_pitch, LANES), jnp.float32)

    def greet():
        barrier = pltpu.get_barrier_semaphore()
        count = jnp.int32(0)
        for side in range(8):
            count = count + has[side].astype(jnp.int32)

            @pl.when(has[side])
            def _():
                pl.semaphore_signal(barrier, inc=1, device_id=neighbour(side), device_id_type=MESH)

        return barrier, count

    def fine_place(g, b, side, arrives):
        if side >= 2:
            return (column_in if arrives else column_out).at[g, min(b, 1), side - 2]
        if b == 2:
            if arrives:
                return row_in.at[g, side]
            return final.at[g, pl.ds(at(0) if side == 0 else at(height - 1), width), :]
        inner, outer = (0, -1) if side == 0 else (height - 1, height)
        return fine.at[g, b, pl.ds(at(outer if arrives else inner), width), :]

    def fine_copy(g, b, side):
        return pltpu.make_async_remote_copy(
            src_ref=fine_place(g, b, side, False), dst_ref=fine_place(g, b, OPPOSITE[side], True),
            send_sem=fine_send.at[g, min(b, 1), side], recv_sem=fine_recv.at[g, min(b, 1), OPPOSITE[side]],
            device_id=neighbour(side), device_id_type=MESH,
        )

    def fine_arrival(g, b, side):
        place = fine_place(g, b, side, True)
        return pltpu.make_async_remote_copy(
            src_ref=place, dst_ref=place,
            send_sem=fine_send.at[g, min(b, 1), OPPOSITE[side]], recv_sem=fine_recv.at[g, min(b, 1), side],
            device_id=neighbour(side), device_id_type=MESH,
        )

    def values_of(g, b):
        return final.at[g] if b == 2 else fine.at[g, b]

    def send_rows(g, b):
        for side in (0, 1):
            pl.when(has[side])(lambda side=side: fine_copy(g, b, side).start())

    def send_columns(g, b):
        ref = values_of(g, b)
        for side, x in ((2, 0), (3, width - 1)):
            out = column_out.at[g, min(b, 1), side - 2]
            for i in range(height // 8):
                out[pl.ds(8 * i, 8), :] = ref[pl.ds(at(8 * i) + x, 8, stride=pitch), :]
        for side in (2, 3):
            pl.when(has[side])(lambda side=side: fine_copy(g, b, side).start())

    def sent_fine(g, b):
        for side in range(4):
            pl.when(has[side])(lambda side=side: fine_copy(g, b, side).wait_send())

    def receive_fine(g, b):
        ref = values_of(g, b)
        for side in (2, 3, 0, 1):
            pl.when(has[side])(lambda side=side: fine_arrival(g, b, side).wait_recv())
        for side, x in ((2, -1), (3, width)):

            @pl.when(has[side])
            def _():
                column = column_in.at[g, min(b, 1), side - 2]
                for i in range(height // 8):
                    ref[pl.ds(at(8 * i) + x, 8, stride=pitch), :] = column[pl.ds(8 * i, 8), :]

    rows = 8
    chunks = height // rows

    def fine_chunk(g, b, i, finish):
        ref = fine.at[g, b]
        top = i * rows
        for p in range(width // part):
            centre = [
                ref[pl.ds(pl.multiple_of(at(top + r - 1) + p * part, 8), part), :]
                for r in range(rows + 2)
            ]
            for r in range(rows):
                here = at(top + r) + p * part
                around = (centre[r] + centre[r + 2]) + (
                    ref[pl.ds(here - 1, part), :] + ref[pl.ds(here + 1, part), :]
                )
                flat = pl.multiple_of((top + r) * width + p * part, 8)
                finish(top, r, p, pl.multiple_of(here, 8), flat, centre[r + 1], around)

    def fine_loop(g, b, finish, between):
        @pl.loop(0, 2)
        def _(i):
            fine_chunk(g, b, i * (chunks - 1), finish)

        between()

        @pl.loop(1, chunks - 1)
        def _(i):
            fine_chunk(g, b, i, finish)

    def sweep_fine(g, b, new):
        out = values_of(g, new)

        def finish(top, r, p, here, flat, centre, around):
            total = load[g, pl.ds(flat, part), :] + around
            out[pl.ds(here, part), :] = KEEP * centre + coef[g, pl.ds(flat, part), :] * total

        fine_loop(g, b, finish, lambda: send_rows(g, new))
        send_columns(g, new)

    def defect(g, flat, centre, around):
        return (load[g, pl.ds(flat, part), :] + around) - (4.0 + mass[g, pl.ds(flat, part), :]) * centre

    def halve(ref, slot, pair):
        scratch = ref.at[slot]
        scratch[...] = pair
        return scratch[pl.ds(0, part // 2, stride=2), :] + scratch[pl.ds(1, part // 2, stride=2), :]

    def coarsen_mass(g):
        step = 4

        @pl.loop(0, height // step)
        def _(i):
            for p in range(width // part):
                for r in range(0, step, 2):
                    pair = []
                    for s in range(2):
                        flat = pl.multiple_of((i * step + r + s) * width + p * part, 8)
                        here = mass[g, pl.ds(flat, part), :]
                        coef[g, pl.ds(flat, part), :] = WEIGHT / (4.0 + here)
                        pair.append(here)
                    summed = 0.5 * halve(temp, p * (step // 2) + r // 2, pair[0] + pair[1])
                    place = coarse_at(i * (step // 2) + r // 2) + p * (part // 2)
                    coarse_coef[g, pl.ds(pl.multiple_of(place, 8), part // 2), :] = WEIGHT / (4.0 + summed)

    def coarsen_defect(g, b):
        held = {}

        def finish(top, r, p, here, flat, centre, around):
            value = defect(g, flat, centre, around)
            if r % 2 == 0:
                held[p] = value
            else:
                summed = 0.5 * halve(temp, p * 4 + r // 2, held[p] + value)
                place = coarse_at(top // 2 + r // 2) + p * (part // 2)
                coarse_load[g, pl.ds(pl.multiple_of(place, 8), part // 2), :] = summed

        fine_loop(g, b, finish, lambda: send_coarse(g, 1, DEPTHS[0], coarse_load.at[g], (4, 5, 6, 7, 0, 1)))
        send_coarse(g, 1, DEPTHS[0], coarse_load.at[g], (2, 3))

    def blocks(side, depth):
        corner = depth - 1
        dy, dx = OFFSETS[side]
        if dx == 0:
            return (depth, w, 0 if dy < 0 else h - depth, 0, -depth if dy < 0 else h, 0)
        if dy == 0:
            return (h, depth, 0, 0 if dx < 0 else w - depth, 0, -depth if dx < 0 else w)
        return (
            corner, corner, 0 if dy < 0 else h - corner, 0 if dx < 0 else w - corner,
            -corner if dy < 0 else h, -corner if dx < 0 else w,
        )

    def buffers(g, e, side, depth):
        rows, columns = blocks(side, depth)[:2]
        if side < 4:
            return (
                edge_out.at[g, e, side, pl.ds(0, rows * columns), :],
                edge_in.at[g, e, side, pl.ds(0, rows * columns), :],
                edge_in.at[g, e, OPPOSITE[side], pl.ds(0, rows * columns), :],
            )
        return (
            corner_out.at[g, e, side - 4, pl.ds(0, rows * columns), :],
            corner_in.at[g, e, side - 4, pl.ds(0, rows * columns), :],
            corner_in.at[g, e, OPPOSITE[side] - 4, pl.ds(0, rows * columns), :],
        )

    def move(rows, columns, source, source_at, target, target_at):
        step = 8
        if rows % step == 0:

            @pl.loop(0, rows // step)
            def _(i):
                for r in range(step):
                    y = i * step + r
                    target[pl.ds(target_at(y), columns), :] = source[pl.ds(source_at(y), columns), :]
        else:
            for y in range(rows):
                target[pl.ds(target_at(y), columns), :] = source[pl.ds(source_at(y), columns), :]

    def slot(e):
        return 0 if e == 0 else 1 + (e - 1) % 2

    def sides_of(depth):
        return range(8 if depth > 1 else 4)

    def coarse_copy(g, e, side, depth):
        out, _, there = buffers(g, e, side, depth)
        return pltpu.make_async_remote_copy(
            src_ref=out, dst_ref=there,
            send_sem=coarse_send.at[g, slot(e), side], recv_sem=coarse_recv.at[g, slot(e), OPPOSITE[side]],
            device_id=neighbour(side), device_id_type=MESH,
        )

    def coarse_arrival(g, e, side, depth):
        _, here, _ = buffers(g, e, side, depth)
        return pltpu.make_async_remote_copy(
            src_ref=here, dst_ref=here,
            send_sem=coarse_send.at[g, slot(e), OPPOSITE[side]], recv_sem=coarse_recv.at[g, slot(e), side],
            device_id=neighbour(side), device_id_type=MESH,
        )

    def send_coarse(g, e, depth, ref, sides=(4, 5, 6, 7, 0, 1, 2, 3)):
        sides = [side for side in sides if side in sides_of(depth)]
        for side in sides:
            rows, columns, y0, x0, _, _ = blocks(side, depth)
            out = edge_out.at[g, e, side] if side < 4 else corner_out.at[g, e, side - 4]
            move(rows, columns, ref, lambda y: coarse_at(y0 + y) + x0, out, lambda y: y * columns)
        for side in sides:
            pl.when(has[side])(lambda side=side: coarse_copy(g, e, side, depth).start())

    def receive_coarse(g, e, depth, ref):
        for side in (2, 3, *range(4, len(sides_of(depth))), 0, 1):

            @pl.when(has[side])
            def _():
                coarse_arrival(g, e, side, depth).wait_recv()
                rows, columns, _, _, y1, x1 = blocks(side, depth)
                held = edge_in.at[g, e, side] if side < 4 else corner_in.at[g, e, side - 4]
                move(rows, columns, held, lambda y: y * columns, ref, lambda y: coarse_at(y1 + y) + x1)

    def sent_coarse(g, e, depth):
        for side in sides_of(depth):
            pl.when(has[side])(lambda side=side: coarse_copy(g, e, side, depth).wait_send())

    def first_coarse(g):
        out = coarse.at[g, 0]

        @pl.loop(0, h + 2 * PAD)
        def _(y):
            here = pl.ds(pl.multiple_of(y * coarse_pitch, 8), coarse_pitch)
            out[here, :] = coarse_coef[g, here, :] * coarse_load[g, here, :]

    def sweep_coarse(g, b, valid):
        ref, out = coarse.at[g, b], coarse.at[g, 1 - b]
        rim = (valid + 1) // 2 * 2
        span, left = (w + 8, -4) if valid else (w, 0)
        rows = 4

        @pl.loop(0, (h + 2 * rim) // rows)
        def _(i):
            top = i * rows - rim
            centre = [ref[pl.ds(coarse_at(top + r - 1) + left, span), :] for r in range(rows + 2)]
            for r in range(rows):
                here = coarse_at(top + r) + left
                around = (centre[r] + centre[r + 2]) + (
                    ref[pl.ds(here - 1, span), :] + ref[pl.ds(here + 1, span), :]
                )
                total = coarse_load[g, pl.ds(here, span), :] + around
                out[pl.ds(here, span), :] = KEEP * centre[r + 1] + coarse_coef[g, pl.ds(here, span), :] * total

    def correct(g, b, c):
        ref, values = fine.at[g, b], coarse.at[g, c]

        def spread(slot, value):
            scratch = temp.at[slot]
            scratch[pl.ds(0, part // 2, stride=2), :] = value
            scratch[pl.ds(1, part // 2, stride=2), :] = value
            return scratch[...]

        def add(y, wide, p):
            here = pl.ds(pl.multiple_of(at(y) + p * part, 8), part)
            ref[here, :] = ref[here, :] + wide

        rows = 4

        @pl.loop(0, h // rows)
        def _(i):
            for r in range(rows):
                for p in range(width // part):
                    place = coarse_at(i * rows + r) + p * (part // 2)
                    wide = spread(r * 2 + p, values[pl.ds(pl.multiple_of(place, 8), part // 2), :])
                    for s in range(2):
                        add((i * rows + r) * 2 + s, wide, p)

        for side, y in ((0, -1), (1, height)):
            for p in range(width // part):
                place = coarse_at(-1 if y < 0 else h) + p * (part // 2)
                add(y, spread(side * 2 + p, values[pl.ds(place, part // 2), :]), p)
        for side, x in ((2, -1), (3, width)):
            for p in range(height // part):
                place = coarse_at(p * (part // 2)) + (-1 if x < 0 else w)
                wide = spread(side * 2 + p, values[pl.ds(place, part // 2, stride=coarse_pitch), :])
                for i in range(part // 8):
                    here = pl.ds(at(p * part + 8 * i) + x, 8, stride=pitch)
                    ref[here, :] = ref[here, :] + wide[8 * i : 8 * i + 8]

    both = range(GROUPS)
    barrier, count = greet()
    for g in both:
        start_values(g)
    for g in both:
        start_terms(g)
    clear_rows()
    pl.semaphore_wait(barrier, count)
    for g in both:
        wait_input(0, g)
        send_rows(g, 0)
        send_columns(g, 0)
    for g in both:
        clear_rest(g)
        wait_input(1, g)
        coarsen_mass(g)
        send_coarse(g, 0, DEPTHS[0], coarse_coef.at[g], PARTS[0])
        wait_input(2, g)
    now = 0
    for sweep in range(BEFORE):
        for g in both:
            receive_fine(g, now)
            if sweep >= 1:
                sent_fine(g, 1 - now)
            sweep_fine(g, now, 1 - now)
            send_coarse(g, 0, DEPTHS[0], coarse_coef.at[g], PARTS[1 + sweep])
        now = 1 - now
    for g in both:
        receive_fine(g, now)
        coarsen_defect(g, now)
    for g in both:
        receive_coarse(g, 0, DEPTHS[0], coarse_coef.at[g])
    inner, c = 1, 0
    for e, depth in enumerate(DEPTHS):
        last = e == len(DEPTHS) - 1
        count = depth - 1 if last else depth
        for g in both:
            b = c
            if e == 0:
                receive_coarse(g, 1, depth, coarse_load.at[g])
                first_coarse(g)
            else:
                receive_coarse(g, 1 + e, depth, coarse.at[g, b])
            for i in range(count):
                sweep_coarse(g, b, depth - 1 - i)
                b = 1 - b
            if not last:
                if e >= 1:
                    sent_coarse(g, e, DEPTHS[e - 1])
                send_coarse(g, 2 + e, DEPTHS[e + 1], coarse.at[g, b])
            else:
                sent_fine(g, now)
                correct(g, now, b)
                sent_fine(g, 1 - now)
                sweep_fine(g, now, 1 - now)
        c = (c + count) % 2
        inner += count
    assert inner == INNER and now == 1
    for g in both:
        receive_fine(g, 0)
        sweep_fine(g, 0, 2)
        for e in (0, len(DEPTHS) - 1, len(DEPTHS)):
            sent_coarse(g, e, DEPTHS[max(e - 1, 0)])
    for g in both:
        receive_fine(g, 2)
        for side, y in ((0, -1), (1, height)):

            @pl.when(has[side])
            def _():
                final[g, pl.ds(at(y), width), :] = row_in[g, side]

        sent_fine(g, 0)
        sent_fine(g, 2)


def finish_kernel(height, width, final, blocked, load, mass, sol_hbm, rem_hbm, rem, sol_sem, rem_sem):
    pitch, part, rows = width + 8, min(32, width), 8
    chunks = 2 if height % (2 * rows) == 0 else 1
    span = height // chunks

    def group_lanes(g):
        return pl.ds(g * LANES, LANES)

    def at(y):
        return (y + 1) * pitch + 8

    def remaining_copy(g, c):
        here = pl.ds(c * span * width, span * width)
        return pltpu.make_async_copy(rem.at[g, here, :], rem_hbm.at[here, group_lanes(g)], rem_sem.at[g, c])

    def solution_copy(g):
        own = blocked.at[g, pl.ds(1, height), pl.ds(8, width), :]
        return pltpu.make_async_copy(own, sol_hbm.at[:, :, group_lanes(g)], sol_sem.at[g])

    for g in range(GROUPS):
        solution_copy(g).start()
    for g in range(GROUPS):
        for c in range(chunks):

            @pl.loop(0, span // rows)
            def _(i):
                top = c * span + i * rows
                for p in range(width // part):
                    centre = [
                        final[g, pl.ds(pl.multiple_of(at(top + r - 1) + p * part, 8), part), :]
                        for r in range(rows + 2)
                    ]
                    for r in range(rows):
                        here = at(top + r) + p * part
                        around = (centre[r] + centre[r + 2]) + (
                            final[g, pl.ds(here - 1, part), :] + final[g, pl.ds(here + 1, part), :]
                        )
                        flat = pl.ds(pl.multiple_of((top + r) * width + p * part, 8), part)
                        rem[g, flat, :] = (load[g, flat, :] + around) - (4.0 + mass[g, flat, :]) * centre[r + 1]

            remaining_copy(g, c).start()
    for g in range(GROUPS):
        for c in range(chunks):
            remaining_copy(g, c).wait()
        solution_copy(g).wait()


def body(load_terms, start_values, reaction_rate):
    height, width, layers = load_terms.shape
    h, w = height // 2, width // 2
    flat = (height * width, layers)
    fine_rows = (height + 3) * (width + 8)
    coarse_rows = (h + 2 * PAD) * (w + 16)
    exchanges = len(DEPTHS) + 1
    edge = max(DEPTHS) * max(h, w) + 8
    corner = -(-((max(DEPTHS) - 1) ** 2) // 8) * 8 + 8
    f32 = jnp.float32
    any_space = pl.BlockSpec(memory_space=pl.ANY)
    vmem_space = pl.BlockSpec(memory_space=pltpu.VMEM)
    cells = height * width
    held = pl.pallas_call(
        functools.partial(kernel, height, width),
        out_shape=[
            pltpu.VMEM((GROUPS, fine_rows, LANES), f32),
            pltpu.VMEM((GROUPS, cells, LANES), f32),
            pltpu.VMEM((GROUPS, cells, LANES), f32),
        ],
        in_specs=[any_space] * 3,
        out_specs=[vmem_space] * 3,
        scratch_shapes=[
            pltpu.VMEM((GROUPS, 2, fine_rows, LANES), f32),
            pltpu.VMEM((GROUPS, cells, LANES), f32),
            pltpu.VMEM((GROUPS, 2, width, LANES), f32),
            pltpu.VMEM((GROUPS, 2, 2, height, LANES), f32),
            pltpu.VMEM((GROUPS, 2, 2, height, LANES), f32),
            pltpu.VMEM((GROUPS, 2, coarse_rows, LANES), f32),
            pltpu.VMEM((GROUPS, coarse_rows, LANES), f32),
            pltpu.VMEM((GROUPS, coarse_rows, LANES), f32),
            pltpu.VMEM((GROUPS, exchanges, 4, edge, LANES), f32),
            pltpu.VMEM((GROUPS, exchanges, 4, edge, LANES), f32),
            pltpu.VMEM((GROUPS, exchanges, 4, corner, LANES), f32),
            pltpu.VMEM((GROUPS, exchanges, 4, corner, LANES), f32),
            pltpu.VMEM((8, min(32, width), LANES), f32),
            pltpu.SemaphoreType.DMA((3, GROUPS)),
            pltpu.SemaphoreType.DMA((GROUPS, 2, 4)),
            pltpu.SemaphoreType.DMA((GROUPS, 2, 4)),
            pltpu.SemaphoreType.DMA((GROUPS, 3, 8)),
            pltpu.SemaphoreType.DMA((GROUPS, 3, 8)),
        ],
        compiler_params=pltpu.CompilerParams(
            collective_id=0, has_side_effects=True, vmem_limit_bytes=48 * 1024 * 1024
        ),
    )(load_terms.reshape(flat), start_values.reshape(flat), reaction_rate.reshape(flat))
    results = pl.pallas_call(
        functools.partial(finish_kernel, height, width),
        out_shape=[
            jax.ShapeDtypeStruct((height, width, layers), f32),
            jax.ShapeDtypeStruct(flat, f32),
        ],
        in_specs=[vmem_space] * 4,
        out_specs=[any_space] * 2,
        scratch_shapes=[
            pltpu.VMEM((GROUPS, cells, LANES), f32),
            pltpu.SemaphoreType.DMA((GROUPS,)),
            pltpu.SemaphoreType.DMA((GROUPS, 2)),
        ],
        compiler_params=pltpu.CompilerParams(vmem_limit_bytes=24 * 1024 * 1024),
    )(held[0], held[0].reshape(GROUPS, height + 3, width + 8, LANES), held[1], held[2])
    return tuple(result.reshape(height, width, layers) for result in results)


def solution(mesh):
    spec = P("band", "lane", None)
    return jax.shard_map(
        body, mesh=mesh, in_specs=(spec, spec, spec), out_specs=(spec, spec), check_vma=False
    )
```
